32 devices in a mesh: sub: 4 (over y, x), rng: 8 (over z, core).
Axes of the slice: x: 2, y: 2, z: 4, core: 2. Of those that a mesh axis runs over, the one named last changes fastest.
Arguments:
- echoes: float32 [512, 2, 12288], P(('sub', 'rng')), may hold values from -6 to 6
- filter_spectrum: float32 [2, 12288], replicated, may hold values from -3 to 3
- range_shifts: int32 [512], P('sub'), may hold values from -16 to 16
- steering: bfloat16 [4, 2, 384, 128], P('sub'), may hold values from -0.375 to 0.375
- tap_offsets: int32 [4, 2, 384], P('sub'), may hold values from -3 to 3
- tap_weights: float32 [4, 2, 4, 384], P('sub'), may hold values from -2 to 2
- phase_rates: float32 [4, 2, 384], P('sub'), may hold values from -6 to 6
Outputs:
- tiles: float32 [1536, 2, 12288], P('sub', None, 'rng')
The draws below stay inside these ranges and needn't reach their ends.
All inputs are finite; a program needn't handle non-finite values.
Results may differ from the reference program's by a relative error of at most 0.0076.
Values may be sent and summed in bfloat16 or wider, within the bound.
No kernel may reach another device: no remote copies, remote signals or barrier semaphores. Data moves between devices by JAX's collectives and lax.ppermute only.
A program may use at most 256 MiB of HBM per device.

```python
import jax
import jax.numpy as jnp
import numpy as np
from jax import lax

ANGLES = 384
TAPS = 4
HALO = 16
SAMPLES = 12288
PSUB = 128
SUBS = 4
PULSES = 512
N_SUB = 4


def touch_ends(entries, key, least, high):
    dims = entries.shape
    spot = [jax.random.randint(jax.random.fold_in(key, axis), (), 0, dims[axis]) for axis in range(len(dims))]
    entries = entries.at[tuple(spot)].set(least)
    longest = dims.index(max(dims))
    spot[longest] = (spot[longest] + 1) % dims[longest]
    return entries.at[tuple(spot)].set(high)


def shard_levels(stream_key, shape, cuts, low, top_value):
    level, own = 1.0, jax.random.fold_in(stream_key, 6)
    for axis_at, shards_of in cuts:
        steps = jnp.exp(jax.random.uniform(jax.random.fold_in(own, axis_at), (shards_of,), jnp.float32, low / len(cuts), top_value / len(cuts)))
        level = level * jnp.repeat(steps, shape[axis_at] // shards_of).reshape([-1 if axis == axis_at else 1 for axis in range(len(shape))])
    return level


def gaussian(key, dims, deviation, most, cuts=(), kind=jnp.bfloat16):
    gain = shard_levels(key, dims, cuts, -0.22, 0.18) if cuts else 1.0
    array = jax.random.normal(key, dims, jnp.float32) * deviation * gain
    return jnp.minimum(jnp.maximum(array, -most), most).astype(kind)


def setup_inputs(seed: int = 0) -> dict:
    arg_keys = jax.random.split(jax.random.key(seed), 8)
    echoes = gaussian(arg_keys[0], (PULSES, 2, SAMPLES), 1.0, 6.0, ((0, 32),), jnp.float32)
    filter_spectrum = gaussian(arg_keys[1], (2, SAMPLES), 0.5, 3.0, (), jnp.float32)
    range_shifts = touch_ends(jax.random.randint(arg_keys[2], (PULSES,), 0 - HALO, HALO + 1), jax.random.fold_in(arg_keys[2], 1), 0 - HALO, HALO).astype(jnp.int32)
    steering = gaussian(arg_keys[3], (SUBS, 2, ANGLES, PSUB), (2 * PSUB) ** -0.5, 0.375, ((0, 4),))
    tap_offsets = touch_ends(jax.random.randint(arg_keys[4], (SUBS, 2, ANGLES), -3, 4), jax.random.fold_in(arg_keys[4], 1), -3, 3).astype(jnp.int32)
    tap_weights = gaussian(arg_keys[5], (SUBS, 2, TAPS, ANGLES), 0.35, 2.0, ((0, 4),), jnp.float32)
    phase_rates = jnp.clip(jax.random.uniform(arg_keys[6], (SUBS, 2, ANGLES), jnp.float32, -6.0, 6.0) * shard_levels(arg_keys[6], (SUBS, 2, ANGLES), ((0, 4),), -0.4, 0.0), -6.0, 6.0)
    return dict(echoes=echoes, filter_spectrum=filter_spectrum, range_shifts=range_shifts, steering=steering, tap_offsets=tap_offsets, tap_weights=tap_weights, phase_rates=phase_rates)


def interp_matrix(weights, offsets):
    angles = jnp.arange(ANGLES, dtype=jnp.int32)
    total = jnp.zeros((ANGLES, ANGLES), jnp.float32)
    for tap in range(TAPS):
        source = jnp.clip(angles + offsets + (tap - 1), 0, ANGLES - 1)
        total = total + weights[tap][:, None] * (angles[None, :] == source[:, None]).astype(jnp.float32)
    return total.astype(jnp.bfloat16)


def rotate(values, phase):
    cosine = jnp.cos(phase)
    sine = jnp.sin(phase)
    real = values[..., 0, :]
    imag = values[..., 1, :]
    return jnp.stack([real * cosine - imag * sine, real * sine + imag * cosine], axis=-2)


def one_group(inputs):
    echo, shifts, steer, spectrum = inputs
    signal = echo[:, 0] + 1j * echo[:, 1]
    filt = spectrum[0] + 1j * spectrum[1]
    out = jnp.fft.ifft(jnp.fft.fft(signal, axis=1) * filt[None, :], axis=1)
    compressed = jnp.stack([jnp.real(out), jnp.imag(out)], axis=1).astype(jnp.float32)
    padded = jnp.pad(compressed, ((0, 0), (0, 0), (HALO, HALO)))

    def cut(row, shift):
        return lax.dynamic_slice_in_dim(row, (HALO + shift).astype(jnp.int32), SAMPLES, 1)

    shifted = jax.vmap(cut)(padded, shifts).astype(jnp.bfloat16)
    mixed = jnp.dot(steer.reshape(2 * ANGLES, PSUB), shifted.reshape(PSUB, 2 * SAMPLES), preferred_element_type=jnp.float32)
    mixed = mixed.reshape(2, ANGLES, 2, SAMPLES)
    real = mixed[0, :, 0] - mixed[1, :, 1]
    imag = mixed[0, :, 1] + mixed[1, :, 0]
    return jnp.stack([real, imag], axis=1).astype(jnp.bfloat16)


def reference(echoes, filter_spectrum, range_shifts, steering, tap_offsets, tap_weights, phase_rates):
    spectra = jnp.broadcast_to(filter_spectrum, (N_SUB, 2, SAMPLES))
    image = lax.map(one_group, (echoes.reshape(N_SUB, PSUB, 2, SAMPLES), range_shifts.reshape(N_SUB, PSUB), steering, spectra))
    mats = jax.vmap(jax.vmap(interp_matrix))(tap_weights, tap_offsets)
    positions = jnp.arange(SAMPLES, dtype=jnp.float32) / SAMPLES
    levels = N_SUB.bit_length() - 1
    merged = None
    for level in range(levels):
        order = np.arange(N_SUB) ^ (1 << level)
        partner = image[order]
        scale = float(level + 1)
        own_part = jnp.einsum("iab,ibc->iac", mats[:, 0].astype(jnp.float32), image.reshape(N_SUB, ANGLES, 2 * SAMPLES).astype(jnp.float32)).reshape(N_SUB, ANGLES, 2, SAMPLES)
        far_part = jnp.einsum("iab,ibc->iac", mats[:, 1].astype(jnp.float32), partner.reshape(N_SUB, ANGLES, 2 * SAMPLES).astype(jnp.float32)).reshape(N_SUB, ANGLES, 2, SAMPLES)
        merged = rotate(own_part, phase_rates[:, 0][:, :, None] * scale * positions[None, None, :]) + rotate(far_part, phase_rates[:, 1][:, :, None] * scale * positions[None, None, :])
        image = merged.astype(jnp.bfloat16)
    return merged.reshape(N_SUB * ANGLES, 2, SAMPLES)
```

```python
import functools
import math

import jax
import jax.numpy as jnp
import numpy as np
from jax import lax
from jax.experimental import pallas as pl
from jax.experimental.pallas import tpu as pltpu
from jax.sharding import PartitionSpec as P


LANES = 128
QUAD = 4
F32 = jnp.float32
BF16 = jnp.bfloat16
VMEM_LIMIT = 60 * 1024 * 1024


def split_table(table):
    high = table.astype(np.float32).astype(BF16)
    low = (table - high.astype(np.float64)).astype(np.float32).astype(BF16)
    return np.stack([high, low])


@functools.lru_cache(None)
def dft_tables(samples):
    radix = samples // LANES
    outer = 2.0 * np.pi * (np.outer(np.arange(radix), np.arange(radix)) % radix) / radix
    inner = 2.0 * np.pi * (np.outer(np.arange(LANES), np.arange(LANES)) % LANES) / LANES
    turn = 2.0 * np.pi * np.outer(np.arange(radix), np.arange(LANES)) / samples
    c, s = np.cos(outer), np.sin(outer)
    first = np.concatenate(
        [np.stack([c, s], -1).reshape(radix, -1), np.stack([-s, c], -1).reshape(radix, -1)]
    )
    last = np.block([[c, -s], [s, c]]) / samples
    c, s = np.cos(inner), np.sin(inner)
    forward = np.block([[c, -s], [s, c]])
    backward = np.block([[c, s], [-s, c]])
    twiddle = np.stack([np.cos(turn), np.sin(turn)]).astype(np.float32)
    return (
        split_table(first),
        split_table(forward),
        split_table(backward),
        split_table(last),
        twiddle,
    )


def halves(x):
    high = x.astype(BF16)
    return high, (x - high.astype(F32)).astype(BF16)


def dot(a, b):
    return jnp.dot(a, b, preferred_element_type=F32)


def table_dot(table, x):
    high, low = halves(x)
    return dot(table[0], high) + dot(table[0], low) + dot(table[1], high)


def dot_table(x, table):
    high, low = halves(x)
    return dot(high, table[0]) + dot(low, table[0]) + dot(high, table[1])


def compress_kernel(ranks, cuts, me_ref, shifts_ref, echo_ref, filt_ref, first_ref, forward_ref, backward_ref, last_ref, twiddle_ref, *refs):
    outs, total = refs[:-1], refs[-1]
    pulses, radix = echo_ref.shape[0], echo_ref.shape[1] // 2
    wide = 2 * pulses
    me = me_ref[0]
    lane = lax.broadcasted_iota(jnp.int32, (radix, LANES), 1)
    row = lax.broadcasted_iota(jnp.int32, (radix, LANES), 0)

    @pl.loop(0, pulses // QUAD)
    def _(step):
        base = step * QUAD
        x = jnp.concatenate([echo_ref[base + q] for q in range(QUAD)], axis=1)
        y = table_dot(first_ref, x)
        wr, wi = twiddle_ref[0], twiddle_ref[1]
        rows = []
        for q in range(QUAD):
            re = y[:radix, q * LANES : (q + 1) * LANES]
            im = y[radix:, q * LANES : (q + 1) * LANES]
            rows.append(jnp.concatenate([re * wr + im * wi, im * wr - re * wi], axis=1))
        z = dot_table(jnp.concatenate(rows, axis=0), forward_ref)
        hr, hi = filt_ref[0], filt_ref[1]
        rows = []
        for q in range(QUAD):
            re = z[q * radix : (q + 1) * radix, :LANES]
            im = z[q * radix : (q + 1) * radix, LANES:]
            rows.append(jnp.concatenate([re * hr - im * hi, re * hi + im * hr], axis=1))
        z = dot_table(jnp.concatenate(rows, axis=0), backward_ref)
        columns = []
        for q in range(QUAD):
            re = z[q * radix : (q + 1) * radix, :LANES]
            im = z[q * radix : (q + 1) * radix, LANES:]
            columns.append(jnp.concatenate([re * wr - im * wi, re * wi + im * wr], axis=0))
        y = table_dot(last_ref, jnp.concatenate(columns, axis=1))
        for q in range(QUAD):
            pulse = base + q
            shift = shifts_ref[me * pulses + pulse]
            source = lane + shift
            for part in range(2):
                cells = y[part * radix : (part + 1) * radix, q * LANES : (q + 1) * LANES]
                turned = pltpu.roll(cells, lax.rem(LANES - shift, LANES), 1)
                after = jnp.where(row == radix - 1, 0.0, pltpu.roll(turned, radix - 1, 0))
                before = jnp.where(row == 0, 0.0, pltpu.roll(turned, 1, 0))
                moved = jnp.where(source >= LANES, after, jnp.where(source < 0, before, turned))
                total[pl.ds(part * pulses + pulse, radix, stride=wide), :] = moved

    length = radix // ranks * wide
    for d in range(ranks):
        start = pl.multiple_of(lax.bitwise_xor(me, d) * length, 8)
        for cut, (low, high) in enumerate(cuts):
            outs[cut * ranks + d][...] = total[
                pl.ds(start + low * wide, (high - low) * wide), :
            ].astype(BF16)


def compress(echoes, filter_spectrum, range_shifts, me, ranks, cuts):
    pulses, _, samples = echoes.shape
    radix = samples // LANES
    wide = 2 * pulses
    view = echoes.reshape(pulses, 2, radix, LANES).transpose(0, 2, 1, 3)
    view = view.reshape(pulses, 2 * radix, LANES)
    filt = filter_spectrum.reshape(2, LANES, radix).transpose(0, 2, 1)
    first, forward, backward, last, twiddle = dft_tables(samples)
    smem = pl.BlockSpec(memory_space=pltpu.SMEM)
    vmem = pl.BlockSpec(memory_space=pltpu.VMEM)
    return pl.pallas_call(
        functools.partial(compress_kernel, ranks, cuts),
        out_shape=[
            jax.ShapeDtypeStruct(((high - low) * wide, LANES), BF16)
            for low, high in cuts
            for _ in range(ranks)
        ],
        in_specs=[smem, smem] + [vmem] * 7,
        out_specs=[vmem] * (ranks * len(cuts)),
        scratch_shapes=[pltpu.VMEM((radix * wide, LANES), F32)],
        compiler_params=pltpu.CompilerParams(vmem_limit_bytes=32 * 1024 * 1024),
        cost_estimate=pl.CostEstimate(
            flops=pulses * samples * 4000, bytes_accessed=pulses * samples * 12, transcendentals=0
        ),
        name="compress",
    )(me, range_shifts, view, filt, *[jnp.asarray(t) for t in (first, forward, backward, last, twiddle)])


def complex_times(a, b):
    return a[0] * b[0] - a[1] * b[1], a[0] * b[1] + a[1] * b[0]


def prepare_kernel(groups, ranks, rows, samples, me_ref, *refs):
    levels = groups.bit_length() - 1
    steer = refs[:groups]
    params = refs[groups : groups + groups // 2]
    mixes, mats, phasors = refs[groups + groups // 2 :]
    angles = mats.shape[-1]
    members = steer[0].shape[-1]
    me = me_ref[0]
    share = members // ranks
    column = lax.broadcasted_iota(jnp.int32, (members, 2 * members), 1)
    member = lax.broadcasted_iota(jnp.int32, (members, 2 * members), 0)
    slot = lax.div(column, 2 * share)
    within = lax.rem(column, 2 * share)
    part = lax.div(within, share)
    source = lax.bitwise_xor(slot, me) * share + lax.rem(within, share)
    picks = [
        jnp.where((part == c) & (source == member), 1.0, 0.0).astype(BF16) for c in range(2)
    ]
    below = lax.broadcasted_iota(jnp.int32, (angles, angles), 0)
    across = lax.broadcasted_iota(jnp.int32, (1, angles), 1)
    lane = lax.broadcasted_iota(jnp.int32, (angles, LANES), 1)
    block = rows * LANES
    at = (me * block + lane).astype(F32) * (1.0 / samples)
    for pick in range(groups // 2):
        offset = 2 * pick
        for h in range(2):
            table = params[pick]
            moved = table[8 + h : 9 + h, :].astype(jnp.int32)
            total = jnp.zeros((angles, angles), F32)
            for tap in range(4):
                at_row = jnp.clip(across + moved + (tap - 1), 0, angles - 1)
                total = total + jnp.where(below == at_row, table[4 * h + tap : 4 * h + tap + 1, :], 0.0)
            matrix = jnp.transpose(total).astype(BF16)
            mats[2 * pick + h] = matrix
            near = steer[offset ^ h]
            real = dot(matrix, near[:angles, :]).astype(BF16)
            imag = dot(matrix, near[angles:, :]).astype(BF16)
            mixes[2 * pick + h, :angles, :] = (dot(real, picks[0]) - dot(imag, picks[1])).astype(BF16)
            mixes[2 * pick + h, angles:, :] = (dot(imag, picks[0]) + dot(real, picks[1])).astype(BF16)
            rate = jnp.transpose(jnp.broadcast_to(table[10 + h : 11 + h, :], (LANES, angles)))
            phase = rate * at
            phasors[2 * pick + h, 0] = jnp.cos(phase)
            phasors[2 * pick + h, 1] = jnp.sin(phase)
            phase = rate * (LANES / samples)
            phasors[2 * pick + h, 2] = jnp.cos(phase)
            phasors[2 * pick + h, 3] = jnp.sin(phase)


def prepare(steer, params, me, groups, ranks, rows, samples):
    angles, members = steer[0].shape[0] // 2, steer[0].shape[1]
    smem = pl.BlockSpec(memory_space=pltpu.SMEM)
    vmem = pl.BlockSpec(memory_space=pltpu.VMEM)
    return pl.pallas_call(
        functools.partial(prepare_kernel, groups, ranks, rows, samples),
        out_shape=[
            jax.ShapeDtypeStruct((groups, 2 * angles, 2 * members), BF16),
            jax.ShapeDtypeStruct((groups, angles, angles), BF16),
            jax.ShapeDtypeStruct((groups, 4, angles, LANES), F32),
        ],
        in_specs=[smem] + [vmem] * (len(steer) + len(params)),
        out_specs=[vmem] * 3,
        compiler_params=pltpu.CompilerParams(vmem_limit_bytes=32 * 1024 * 1024),
        cost_estimate=pl.CostEstimate(
            flops=groups * angles * members * 40000, bytes_accessed=8 << 20, transcendentals=0
        ),
        name="prepare",
    )(me, *steer, *params)


BAND = 32


def merge_kernel(groups, layout, first, count, mixes, mats, phasors, *refs):
    levels = groups.bit_length() - 1
    parts = refs[: sum(len(p) for p in layout)]
    out = refs[len(parts)]
    current, strides, mixed, image = refs[len(parts) + 1 :]
    held, at = [], 0
    for sizes in layout:
        held.append(parts[at : at + len(sizes)])
        at += len(sizes)
    angles = mats.shape[-1]
    wide = held[0][0].shape[1] // count
    rows = out.shape[0] // angles // 2
    pair = 2 if count % 2 == 0 else 1
    for n in range(groups):
        for top in range(0, angles, BAND):
            band = slice(top, top + BAND)
            turn = (phasors[n, 2, band], phasors[n, 3, band])
            now = (phasors[n, 0, band], phasors[n, 1, band])
            jump = turn
            for u in range(pair):
                here = slice(u * LANES, (u + 1) * LANES)
                current[n, 0, band, here], current[n, 1, band, here] = now
                if u < pair - 1:
                    now = complex_times(now, turn)
                    jump = complex_times(jump, turn)
            strides[n, 0, band], strides[n, 1, band] = jump

    def column(offset, j):
        return jnp.concatenate(
            [
                ref[:, pl.ds(pl.multiple_of(j * wide, 8), wide), :].reshape(-1, LANES)
                for ref in held[offset]
            ],
            axis=0,
        )

    @pl.loop(0, count // pair)
    def _(step):
        base = step * pair
        cells = [
            jnp.concatenate([column(offset, base + u) for u in range(pair)], axis=1)
            for offset in range(groups)
        ]
        for n in range(groups):
            pick, h = n // 2, n % 2
            mixed[n] = dot(mixes[n], cells[(2 * pick) ^ h])
        for level in range(levels):
            last = level == levels - 1
            stride = 2 << level
            if level:
                for offset in range(0, groups, stride):
                    for h in range(2):
                        n = offset + h
                        far = offset ^ (h << level)
                        mixed_out = dot(mats[n], image[far // 2])
                        mixed[n, :angles] = mixed_out[:, : pair * LANES]
                        mixed[n, angles:] = mixed_out[:, pair * LANES :]
            for offset in range(0, groups, stride):
                for top in range(0, angles, BAND):
                    band = slice(top, top + BAND)
                    lower = slice(angles + top, angles + top + BAND)
                    for u in range(pair):
                        here = slice(u * LANES, (u + 1) * LANES)
                        terms = []
                        for h in range(2):
                            n = offset + h
                            now = (current[n, 0, band, here], current[n, 1, band, here])
                            power = now
                            for _ in range(level):
                                power = complex_times(power, now)
                            terms.append(
                                complex_times((mixed[n, band, here], mixed[n, lower, here]), power)
                            )
                            if last or offset % (2 * stride):
                                jump = (strides[n, 0, band], strides[n, 1, band])
                                moved = complex_times(now, jump)
                                current[n, 0, band, here], current[n, 1, band, here] = moved
                        re = terms[0][0] + terms[1][0]
                        im = terms[0][1] + terms[1][1]
                        if last:
                            spot = (first + base + u) * 2
                            out[pl.ds(top * rows * 2 + spot, BAND, stride=rows * 2), :] = re
                            out[pl.ds(top * rows * 2 + spot + 1, BAND, stride=rows * 2), :] = im
                        else:
                            image[offset // 2, band, here] = re.astype(BF16)
                            far_side = slice((pair + u) * LANES, (pair + u + 1) * LANES)
                            image[offset // 2, band, far_side] = im.astype(BF16)


def gather(x, groups):
    def hop(value, bit):
        return lax.ppermute(value, "sub", [(i, i ^ bit) for i in range(groups)])

    held = {0: [x]}
    bits = [1 << b for b in range(groups.bit_length() - 1)]
    for bit in bits:
        held[bit] = [hop(x, bit)]
    return held, hop, bits


def full_gather(x, groups):
    held, hop, bits = gather(x, groups)
    slots = x.shape[0]
    for offset in range(3, groups):
        if offset in held:
            continue
        via = [bit for bit in bits if offset & bit]
        edges = [slots * i // len(via) for i in range(len(via) + 1)]
        pieces = []
        for bit, low, high in zip(via, edges[:-1], edges[1:]):
            near = held[offset ^ bit]
            near = near[0] if len(near) == 1 else jnp.concatenate(near, axis=0)
            pieces.append(hop(near[low:high], bit))
        held[offset] = pieces
    return [held[offset] for offset in range(groups)]


def merge(held, mixes, mats, phasors, rows):
    groups, angles = mats.shape[0], mats.shape[-1]
    pair = 2 if rows % 2 == 0 else 1
    layout = [[part.shape[0] for part in parts] for parts in held]
    flat = [part for parts in held for part in parts]
    vmem = pl.BlockSpec(memory_space=pltpu.VMEM)
    return pl.pallas_call(
        functools.partial(merge_kernel, groups, layout, 0, rows),
        out_shape=jax.ShapeDtypeStruct((angles * rows * 2, LANES), F32),
        in_specs=[vmem] * (3 + len(flat)),
        out_specs=vmem,
        scratch_shapes=[
            pltpu.VMEM((groups, 2, angles, pair * LANES), F32),
            pltpu.VMEM((groups, 2, angles, LANES), F32),
            pltpu.VMEM((groups, 2 * angles, pair * LANES), F32),
            pltpu.VMEM((max(groups // 2, 1), angles, 2 * pair * LANES), BF16),
        ],
        compiler_params=pltpu.CompilerParams(vmem_limit_bytes=VMEM_LIMIT),
        cost_estimate=pl.CostEstimate(
            flops=groups * angles * angles * rows * LANES * 8,
            bytes_accessed=angles * rows * LANES * 16,
            transcendentals=0,
        ),
        name="merge",
    )(mixes, mats, phasors, *flat)


def local(echoes, filter_spectrum, range_shifts, steering, tap_offsets, tap_weights, phase_rates):
    ranks, groups = lax.axis_size("rng"), lax.axis_size("sub")
    samples = echoes.shape[2]
    rows = samples // LANES // ranks
    angles = steering.shape[2]
    me = lax.axis_index("rng").astype(jnp.int32).reshape(1)

    blocks = compress(echoes, filter_spectrum, range_shifts, me, ranks, [(0, rows)])
    received = [blocks[0]]
    for d in range(1, ranks):
        received.append(lax.ppermute(blocks[d], "rng", [(i, i ^ d) for i in range(ranks)]))

    params = jnp.concatenate(
        [
            tap_weights.reshape(-1, angles),
            tap_offsets.reshape(2, angles).astype(F32),
            phase_rates.reshape(2, angles),
            jnp.zeros((4, angles), F32),
        ],
        axis=0,
    )
    steer = steering.reshape(2 * angles, -1)
    steer, params, _ = lax.optimization_barrier((steer, params, blocks[1]))

    def far(value, offset):
        if not offset:
            return value
        return lax.ppermute(value, "sub", [(i, i ^ offset) for i in range(groups)])

    mixes, mats, phasors = prepare(
        [far(steer, e) for e in range(groups)],
        [far(params, e) for e in range(0, groups, 2)],
        me,
        groups,
        ranks,
        rows,
        samples,
    )
    held = full_gather(jnp.stack(received), groups)
    out = merge(held, mixes, mats, phasors, rows)
    out = out.reshape(angles, rows, 2, LANES).transpose(0, 2, 1, 3)
    return out.reshape(angles, 2, rows * LANES)


def solution(mesh):
    placed = (
        P(("sub", "rng"), None, None),
        P(),
        P("sub"),
        P("sub", None, None, None),
        P("sub", None, None),
        P("sub", None, None, None),
        P("sub", None, None),
    )
    return jax.shard_map(
        local, mesh=mesh, in_specs=placed, out_specs=P("sub", None, "rng"), check_vma=False
    )
```

```python
import functools

import jax
import jax.numpy as jnp
import numpy as np
from jax import lax
from jax.experimental import pallas as pl
from jax.experimental.layout import Layout, with_layout_constraint
from jax.experimental.pallas import tpu as pltpu
from jax.sharding import PartitionSpec as P


LANES = 128
QUAD = 4
F32 = jnp.float32
BF16 = jnp.bfloat16
VMEM_LIMIT = 28 * 1024 * 1024
UNIT = 4
SHARE = 4
LOADS = 10
COMPRESS_LIMIT = 60 * 1024 * 1024


def split_table(table):
    high = table.astype(np.float32).astype(BF16)
    low = (table - high.astype(np.float64)).astype(np.float32).astype(BF16)
    return np.stack([high, low])


@functools.lru_cache(None)
def dft_tables(samples):
    radix = samples // LANES
    outer = 2.0 * np.pi * (np.outer(np.arange(radix), np.arange(radix)) % radix) / radix
    inner = 2.0 * np.pi * (np.outer(np.arange(LANES), np.arange(LANES)) % LANES) / LANES
    turn = 2.0 * np.pi * np.outer(np.arange(radix), np.arange(LANES)) / samples
    c, s = np.cos(outer), np.sin(outer)
    first = np.concatenate(
        [np.stack([c, s], -1).reshape(radix, -1), np.stack([-s, c], -1).reshape(radix, -1)]
    )
    last = np.block([[c, -s], [s, c]]) / samples
    c, s = np.cos(inner), np.sin(inner)
    forward = np.block([[c, -s], [s, c]])
    backward = np.block([[c, s], [-s, c]])
    twiddle = np.stack([np.cos(turn), np.sin(turn)]).astype(np.float32)
    return (
        split_table(first),
        split_table(forward),
        split_table(backward),
        split_table(last),
        twiddle,
    )


def halves(x):
    high = x.astype(BF16)
    return high, (x - high.astype(F32)).astype(BF16)


def dot(a, b):
    return jnp.dot(a, b, preferred_element_type=F32)


def table_dot(table, x):
    high, low = halves(x)
    return dot(table[0], high) + dot(table[0], low) + dot(table[1], high)


def dot_table(x, table):
    high, low = halves(x)
    return dot(high, table[0]) + dot(low, table[0]) + dot(high, table[1])


def encode(early, base, taps_ref, offsets_ref, rates_ref):
    angles = rates_ref.shape[1]
    empty = jnp.zeros((16 - taps_ref.shape[0] - 4, angles), F32)
    left = jnp.concatenate(
        [taps_ref[...], offsets_ref[...].astype(F32), rates_ref[...], empty], axis=0
    )
    for piece in range(3):
        high = left.astype(BF16)
        left = left - high.astype(F32)
        for at in range(angles // LANES):
            spot = base + 16 * (piece * (angles // LANES) + at)
            early[spot : spot + 16, :LANES] = high[:, at * LANES : (at + 1) * LANES]


def decode(ref, base, angles):
    pieces = []
    for piece in range(3):
        spots = [base + 16 * (piece * (angles // LANES) + at) for at in range(angles // LANES)]
        pieces.append(
            jnp.concatenate([ref[spot : spot + 16, :LANES] for spot in spots], axis=1).astype(F32)
        )
    return pieces[0] + pieces[1] + pieces[2]


def compress_kernel(ranks, cuts, me_ref, shifts_ref, filt_ref, *refs):
    loads, outs = refs[:LOADS], refs[LOADS : LOADS + len(cuts) + 1]
    early = refs[LOADS + len(cuts) + 1]
    total, *held = refs[LOADS + len(cuts) + 2 : -1]
    done = refs[-1]
    echo_ref, first_ref, forward_ref, backward_ref, last_ref, twiddle_ref = held[:6]
    taps_ref, offsets_ref, rates_ref = held[6:]
    held = [*held, early.at[pl.ds(0, loads[-1].shape[0])]]
    copies = [pltpu.make_async_copy(loads[i], held[i], done.at[i]) for i in range(1, LOADS)]
    pieces = [
        pltpu.make_async_copy(
            loads[0].at[pl.ds(q * QUAD, QUAD)], echo_ref.at[pl.ds(q * QUAD, QUAD)], done.at[LOADS + q]
        )
        for q in range(echo_ref.shape[0] // QUAD)
    ]
    for copy in (copies[0], pieces[0], *copies[1:], *pieces[1:]):
        copy.start()
    for copy in (*copies, *pieces):
        copy.wait()
    encode(early, loads[-1].shape[0], taps_ref, offsets_ref, rates_ref)
    pulses, radix = echo_ref.shape[0], echo_ref.shape[1] // 2
    wide = 2 * pulses
    me = me_ref[0]
    lane = lax.broadcasted_iota(jnp.int32, (radix, LANES), 1)
    row = lax.broadcasted_iota(jnp.int32, (radix, LANES), 0)

    @pl.loop(0, pulses // QUAD)
    def _(step):
        base = step * QUAD
        x = jnp.concatenate([echo_ref[base + q] for q in range(QUAD)], axis=1)
        y = table_dot(first_ref, x)
        wr, wi = twiddle_ref[0], twiddle_ref[1]
        rows = []
        for q in range(QUAD):
            re = y[:radix, q * LANES : (q + 1) * LANES]
            im = y[radix:, q * LANES : (q + 1) * LANES]
            rows.append(jnp.concatenate([re * wr + im * wi, im * wr - re * wi], axis=1))
        z = dot_table(jnp.concatenate(rows, axis=0), forward_ref)
        hr, hi = filt_ref[0], filt_ref[1]
        rows = []
        for q in range(QUAD):
            re = z[q * radix : (q + 1) * radix, :LANES]
            im = z[q * radix : (q + 1) * radix, LANES:]
            rows.append(jnp.concatenate([re * hr - im * hi, re * hi + im * hr], axis=1))
        z = dot_table(jnp.concatenate(rows, axis=0), backward_ref)
        columns = []
        for q in range(QUAD):
            re = z[q * radix : (q + 1) * radix, :LANES]
            im = z[q * radix : (q + 1) * radix, LANES:]
            columns.append(jnp.concatenate([re * wr - im * wi, re * wi + im * wr], axis=0))
        y = table_dot(last_ref, jnp.concatenate(columns, axis=1))
        for q in range(QUAD):
            pulse = base + q
            shift = shifts_ref[me * pulses + pulse]
            source = lane + shift
            for part in range(2):
                cells = y[part * radix : (part + 1) * radix, q * LANES : (q + 1) * LANES]
                turned = pltpu.roll(cells, lax.rem(LANES - shift, LANES), 1)
                after = jnp.where(row == radix - 1, 0.0, pltpu.roll(turned, radix - 1, 0))
                before = jnp.where(row == 0, 0.0, pltpu.roll(turned, 1, 0))
                moved = jnp.where(source >= LANES, after, jnp.where(source < 0, before, turned))
                total[pl.ds(part * pulses + pulse, radix, stride=wide), :] = moved

    length = radix // ranks * wide
    for d in range(ranks):
        start = pl.multiple_of(lax.bitwise_xor(me, d) * length, 8)
        if d % 2:
            outs[-1][d // 2] = total[pl.ds(start, length), :].astype(BF16)
            continue
        for cut, (low, high) in enumerate(cuts):
            cells = total[pl.ds(start + low * wide, (high - low) * wide), :]
            outs[cut][d // 2] = cells.astype(BF16)


def compress(echoes, filter_spectrum, range_shifts, steering, tap_offsets, tap_weights, phase_rates, me, ranks, cuts):
    pulses, _, samples = echoes.shape
    radix = samples // LANES
    wide = 2 * pulses
    view = echoes.reshape(pulses, 2, radix, LANES).transpose(0, 2, 1, 3)
    view = view.reshape(pulses, 2 * radix, LANES)
    filt = filter_spectrum.reshape(2, LANES, radix).transpose(0, 2, 1)
    angles = steering.shape[2]
    steer = steering.reshape(2 * angles, -1)
    loads = [view] + [jnp.asarray(t) for t in dft_tables(samples)]
    loads += [tap_weights.reshape(-1, angles), tap_offsets.reshape(2, angles)]
    loads += [phase_rates.reshape(2, angles), steer]
    smem = pl.BlockSpec(memory_space=pltpu.SMEM)
    vmem = pl.BlockSpec(memory_space=pltpu.VMEM)
    away = pl.BlockSpec(memory_space=pltpu.HBM)
    half = ranks // 2
    return pl.pallas_call(
        functools.partial(compress_kernel, ranks, cuts),
        out_shape=[
            jax.ShapeDtypeStruct((half, (high - low) * wide, LANES), BF16)
            for low, high in [*cuts, (0, radix // ranks)]
        ]
        + [jax.ShapeDtypeStruct((2 * angles + 48 * angles // LANES, steer.shape[1]), BF16)],
        in_specs=[smem, smem, vmem] + [away] * LOADS,
        out_specs=[vmem] * (2 + len(cuts)),
        scratch_shapes=[pltpu.VMEM((radix * wide, LANES), F32)]
        + [pltpu.VMEM(x.shape, x.dtype) for x in loads[:-1]]
        + [pltpu.SemaphoreType.DMA((LOADS + pulses // QUAD,))],
        compiler_params=pltpu.CompilerParams(vmem_limit_bytes=COMPRESS_LIMIT),
        cost_estimate=pl.CostEstimate(
            flops=pulses * samples * 4000, bytes_accessed=pulses * samples * 12, transcendentals=0
        ),
        name="compress",
    )(me, range_shifts, filt, *loads)


def pack_kernel(cuts, wide, *refs):
    near, far, outs = refs[: len(cuts)], refs[len(cuts)], refs[len(cuts) + 1 :]
    half = far.shape[0]
    for cut, (low, high) in enumerate(cuts):
        for z in range(half):
            outs[cut * half + z][0] = near[cut][z]
            outs[cut * half + z][1] = far[z, low * wide : high * wide]


def pack(near, far, cuts, wide):
    half = far.shape[0]
    vmem = pl.BlockSpec(memory_space=pltpu.VMEM)
    flat = pl.pallas_call(
        functools.partial(pack_kernel, cuts, wide),
        out_shape=[
            jax.ShapeDtypeStruct((2, (high - low) * wide, LANES), BF16)
            for low, high in cuts
            for _ in range(half)
        ],
        in_specs=[vmem] * (len(cuts) + 1),
        out_specs=[vmem] * (len(cuts) * half),
        compiler_params=pltpu.CompilerParams(vmem_limit_bytes=16 * 1024 * 1024),
        cost_estimate=pl.CostEstimate(flops=1 << 20, bytes_accessed=1 << 20, transcendentals=0),
        name="pack",
    )(*near, far)
    return [flat[cut * half : (cut + 1) * half] for cut in range(len(cuts))]


def complex_times(a, b):
    return a[0] * b[0] - a[1] * b[1], a[0] * b[1] + a[1] * b[0]


def prepare_kernel(groups, ranks, rows, samples, cuts, me_ref, *refs):
    levels = groups.bit_length() - 1
    steer = refs[:groups]
    mixes, mats, phasors = refs[groups:]
    angles = mats.shape[-1]
    members = steer[0].shape[-1]
    me = me_ref[0]
    share = members // ranks
    column = lax.broadcasted_iota(jnp.int32, (members, 2 * members), 1)
    member = lax.broadcasted_iota(jnp.int32, (members, 2 * members), 0)
    slot = lax.div(column, 2 * share)
    within = lax.rem(column, 2 * share)
    part = lax.div(within, share)
    source = lax.bitwise_xor(slot, me) * share + lax.rem(within, share)
    picks = [
        jnp.where((part == c) & (source == member), 1.0, 0.0).astype(BF16) for c in range(2)
    ]
    below = lax.broadcasted_iota(jnp.int32, (angles, angles), 0)
    across = lax.broadcasted_iota(jnp.int32, (1, angles), 1)
    lane = lax.broadcasted_iota(jnp.int32, (angles, LANES), 1)
    block = rows * LANES
    at = (me * block + lane).astype(F32) * (1.0 / samples)
    for pick in range(groups // 2):
        offset = 2 * pick
        table = decode(steer[offset], 2 * angles, angles)
        for h in range(2):
            moved = table[8 + h : 9 + h, :].astype(jnp.int32)
            total = jnp.zeros((angles, angles), F32)
            for tap in range(4):
                at_row = jnp.clip(across + moved + (tap - 1), 0, angles - 1)
                total = total + jnp.where(below == at_row, table[4 * h + tap : 4 * h + tap + 1, :], 0.0)
            matrix = jnp.transpose(total).astype(BF16)
            mats[2 * pick + h] = matrix
            near = steer[offset ^ h]
            real = dot(matrix, near[:angles, :]).astype(BF16)
            imag = dot(matrix, near[angles : 2 * angles, :]).astype(BF16)
            mixes[2 * pick + h, :angles, :] = (dot(real, picks[0]) - dot(imag, picks[1])).astype(BF16)
            mixes[2 * pick + h, angles:, :] = (dot(imag, picks[0]) + dot(real, picks[1])).astype(BF16)
            rate = jnp.transpose(jnp.broadcast_to(table[10 + h : 11 + h, :], (LANES, angles)))
            n = 2 * pick + h
            phase = rate * at
            now = (jnp.cos(phase), jnp.sin(phase))
            phase = rate * (LANES / samples)
            turn = (jnp.cos(phase), jnp.sin(phase))
            phasors[n, 0], phasors[n, 1] = turn
            for cut, (low, high) in enumerate(cuts):
                phasors[n, 2 + 2 * cut], phasors[n, 3 + 2 * cut] = now
                if high < rows:
                    for _ in range(low, high):
                        now = complex_times(now, turn)


def prepare(steer, angles, me, groups, ranks, rows, samples, cuts):
    members = steer[0].shape[1]
    smem = pl.BlockSpec(memory_space=pltpu.SMEM)
    vmem = pl.BlockSpec(memory_space=pltpu.VMEM)
    return pl.pallas_call(
        functools.partial(prepare_kernel, groups, ranks, rows, samples, cuts),
        out_shape=[
            jax.ShapeDtypeStruct((groups, 2 * angles, 2 * members), BF16),
            jax.ShapeDtypeStruct((groups, angles, angles), BF16),
            jax.ShapeDtypeStruct((groups, 2 + 2 * len(cuts), angles, LANES), F32),
        ],
        in_specs=[smem] + [vmem] * len(steer),
        out_specs=[vmem] * 3,
        compiler_params=pltpu.CompilerParams(vmem_limit_bytes=32 * 1024 * 1024),
        cost_estimate=pl.CostEstimate(
            flops=groups * angles * members * 40000, bytes_accessed=8 << 20, transcendentals=0
        ),
        name="prepare",
    )(me, *steer)


BAND = 32


def merge_kernel(groups, layout, cut, count, unit, mixes, mats, phasors, *refs):
    levels = groups.bit_length() - 1
    parts = refs[: sum(len(p) for p in layout)]
    out, current, strides, mixed, image = refs[-5:]
    held, at = [], 0
    for sizes in layout:
        held.append(parts[at : at + len(sizes)])
        at += len(sizes)
    if len(out.shape) == 3:
        out = out.reshape(out.shape[0] * out.shape[1], LANES)
    angles = mats.shape[-1]
    wide = held[0][0].shape[1] // count
    pair = 2 if unit % 2 == 0 else 1
    started = pl.program_id(0) * unit
    @pl.when(started == 0)
    def _():
        for n in range(groups):
            for top in range(0, angles, BAND):
                band = slice(top, top + BAND)
                turn = (phasors[n, 0, band], phasors[n, 1, band])
                now = (phasors[n, 2 + 2 * cut, band], phasors[n, 3 + 2 * cut, band])
                jump = turn
                for u in range(pair):
                    here = slice(u * LANES, (u + 1) * LANES)
                    current[n, 0, band, here], current[n, 1, band, here] = now
                    if u < pair - 1:
                        now = complex_times(now, turn)
                        jump = complex_times(jump, turn)
                strides[n, 0, band], strides[n, 1, band] = jump

    def column(offset, j):
        return jnp.concatenate(
            [
                ref[:, pl.ds(pl.multiple_of(j * wide, 8), wide), :].reshape(-1, LANES)
                for ref in held[offset]
            ],
            axis=0,
        )

    @pl.loop(0, unit // pair)
    def _(step):
        base = started + step * pair
        cells = [
            jnp.concatenate([column(offset, base + u) for u in range(pair)], axis=1)
            for offset in range(groups)
        ]
        for n in range(groups):
            pick, h = n // 2, n % 2
            mixed[n] = dot(mixes[n], cells[(2 * pick) ^ h])
        for level in range(levels):
            last = level == levels - 1
            stride = 2 << level
            if level:
                for offset in range(0, groups, stride):
                    for h in range(2):
                        n = offset + h
                        far = offset ^ (h << level)
                        mixed_out = dot(mats[n], image[far // 2])
                        mixed[n, :angles] = mixed_out[:, : pair * LANES]
                        mixed[n, angles:] = mixed_out[:, pair * LANES :]
            for offset in range(0, groups, stride):
                for top in range(0, angles, BAND):
                    band = slice(top, top + BAND)
                    lower = slice(angles + top, angles + top + BAND)
                    for u in range(pair):
                        here = slice(u * LANES, (u + 1) * LANES)
                        terms = []
                        for h in range(2):
                            n = offset + h
                            now = (current[n, 0, band, here], current[n, 1, band, here])
                            power = now
                            for _ in range(level):
                                power = complex_times(power, now)
                            terms.append(
                                complex_times((mixed[n, band, here], mixed[n, lower, here]), power)
                            )
                            if last or offset % (2 * stride):
                                jump = (strides[n, 0, band], strides[n, 1, band])
                                moved = complex_times(now, jump)
                                current[n, 0, band, here], current[n, 1, band, here] = moved
                        re = terms[0][0] + terms[1][0]
                        im = terms[0][1] + terms[1][1]
                        if last:
                            spot = top * unit * 2 + (step * pair + u) * 2
                            out[pl.ds(spot, BAND, stride=unit * 2), :] = re
                            out[pl.ds(spot + 1, BAND, stride=unit * 2), :] = im
                        else:
                            image[offset // 2, band, here] = re.astype(BF16)
                            far_side = slice((pair + u) * LANES, (pair + u + 1) * LANES)
                            image[offset // 2, band, far_side] = im.astype(BF16)


def merge(held, mixes, mats, phasors, rows, cut, low, high, unit, before):
    groups, angles = mats.shape[0], mats.shape[-1]
    pair = 2 if unit % 2 == 0 else 1
    layout = [[part.shape[0] for part in parts] for parts in held]
    flat = [part for parts in held for part in parts]
    vmem = pl.BlockSpec(memory_space=pltpu.VMEM)
    if unit * 2 % 8:
        shape, block, spot = (angles * rows * 2, LANES), (angles * unit * 2, LANES), lambda i: (0, 0)
    else:
        shape, block = (angles, rows * 2, LANES), (angles, unit * 2, LANES)
        spot = lambda i: (0, low // unit + i, 0)
    operands = [mixes, mats, phasors, *flat]
    specs = [vmem] * len(operands)
    aliases = {}
    if before is not None:
        aliases = {len(operands): 0}
        operands.append(before)
        specs.append(pl.BlockSpec(memory_space=pltpu.HBM))
    return pl.pallas_call(
        functools.partial(merge_kernel, groups, layout, cut, high - low, unit),
        grid=((high - low) // unit,),
        out_shape=jax.ShapeDtypeStruct(shape, F32),
        in_specs=specs,
        out_specs=pl.BlockSpec(block, spot),
        input_output_aliases=aliases,
        scratch_shapes=[
            pltpu.VMEM((groups, 2, angles, pair * LANES), F32),
            pltpu.VMEM((groups, 2, angles, LANES), F32),
            pltpu.VMEM((groups, 2 * angles, pair * LANES), F32),
            pltpu.VMEM((max(groups // 2, 1), angles, 2 * pair * LANES), BF16),
        ],
        compiler_params=pltpu.CompilerParams(vmem_limit_bytes=VMEM_LIMIT),
        cost_estimate=pl.CostEstimate(
            flops=groups * angles * angles * (high - low) * LANES * 8,
            bytes_accessed=angles * (high - low) * LANES * 16,
            transcendentals=0,
        ),
        name="merge",
    )(*operands)


def hop(value, axis, offset):
    if not offset:
        return value
    return lax.ppermute(value, axis, [(i, i ^ offset) for i in range(lax.axis_size(axis))])


def neighbours(x, groups):
    return {1 << b: hop(x, "sub", 1 << b) for b in range(groups.bit_length() - 1)}


def others(x, near, groups):
    held = {0: [x]}
    for bit in near:
        held[bit] = [near[bit]]
    slots = x.shape[0]
    for offset in range(groups):
        if offset in held:
            continue
        via = [bit for bit in near if offset & bit]
        edges = [slots * i // len(via) for i in range(len(via) + 1)]
        pieces = []
        for bit, low, high in zip(via, edges[:-1], edges[1:]):
            source = held[offset ^ bit]
            source = source[0] if len(source) == 1 else jnp.concatenate(source, axis=0)
            pieces.append(hop(source[low:high], "sub", bit))
        held[offset] = pieces
    return [held[offset] for offset in range(groups)]


def local(echoes, filter_spectrum, range_shifts, steering, tap_offsets, tap_weights, phase_rates):
    ranks, groups = lax.axis_size("rng"), lax.axis_size("sub")
    pulses, _, samples = echoes.shape
    rows = samples // LANES // ranks
    angles = steering.shape[2]
    me = lax.axis_index("rng").astype(jnp.int32).reshape(1)
    unit = UNIT if rows % UNIT == 0 else rows
    edges = sorted({0, unit * (rows // unit * SHARE // 12), rows})
    cuts = list(zip(edges[:-1], edges[1:]))

    *near, odd, early = compress(
        echoes, filter_spectrum, range_shifts, steering, tap_offsets, tap_weights, phase_rates,
        me, ranks, cuts,
    )
    steers = [hop(early, "sub", e) for e in range(groups)]
    packed = pack(near, hop(odd, "rng", 1), cuts, 2 * pulses)
    arrived = [
        jnp.concatenate([hop(block, "rng", 2 * z) for z, block in enumerate(blocks)], axis=0)
        for blocks in packed
    ]
    ready = prepare(steers, angles, me, groups, ranks, rows, samples, cuts)

    nears = []
    for x in arrived:
        nears.append(neighbours(x, groups))
    nears[0], ready = lax.optimization_barrier((nears[0], ready))
    out = None
    for cut, (low, high) in enumerate(cuts):
        held = others(arrived[cut], nears[cut], groups)
        out = merge(held, *ready, rows, cut, low, high, unit, out)
    out = out.reshape(angles, rows, 2, LANES).transpose(0, 2, 1, 3)
    out = with_layout_constraint(out, Layout(major_to_minor=(0, 2, 1, 3)))
    return out.reshape(angles, 2, rows * LANES)


def solution(mesh):
    placed = (
        P(("sub", "rng"), None, None),
        P(),
        P("sub"),
        P("sub", None, None, None),
        P("sub", None, None),
        P("sub", None, None, None),
        P("sub", None, None),
    )
    return jax.shard_map(
        local, mesh=mesh, in_specs=placed, out_specs=P("sub", None, "rng"), check_vma=False
    )
```

```python
import functools
import math

import jax
import jax.numpy as jnp
import numpy as np
from jax import lax
from jax.experimental import pallas as pl
from jax.experimental.layout import Layout, with_layout_constraint
from jax.experimental.pallas import tpu as pltpu
from jax.sharding import PartitionSpec as P


LANES = 128
QUAD = 4
F32 = jnp.float32
BF16 = jnp.bfloat16
VMEM_LIMIT = 28 * 1024 * 1024
UNIT = 4
SHARE = 4
LOADS = 11
PASSES = (3, 3, 1, 1)
COMPRESS_LIMIT = 60 * 1024 * 1024


def split_table(table):
    high = table.astype(np.float32).astype(BF16)
    low = (table - high.astype(np.float64)).astype(np.float32).astype(BF16)
    return np.stack([high, low])


def frequency_order(radix):
    sections = math.lcm(radix, LANES) // radix
    place = np.arange(LANES)
    return sections * (place % (LANES // sections)) + place // (LANES // sections)


@functools.lru_cache(None)
def dft_tables(samples):
    radix = samples // LANES
    outer = 2.0 * np.pi * (np.outer(np.arange(radix), np.arange(radix)) % radix) / radix
    inner = 2.0 * np.pi * (np.outer(np.arange(LANES), np.arange(LANES)) % LANES) / LANES
    turn = 2.0 * np.pi * np.outer(np.arange(radix), np.arange(LANES)) / samples
    c, s = np.cos(outer), np.sin(outer)
    first = np.concatenate(
        [np.stack([c, s], -1).reshape(radix, -1), np.stack([-s, c], -1).reshape(radix, -1)]
    )
    last = np.block([[c, -s], [s, c]]) / samples
    order = frequency_order(radix)
    c, s = np.cos(inner)[:, order], np.sin(inner)[:, order]
    forward = np.block([[c, -s], [s, c]])
    backward = np.block([[c.T, s.T], [-s.T, c.T]])
    twiddle = np.stack([np.cos(turn), np.sin(turn)]).astype(np.float32)
    return (
        split_table(first),
        split_table(forward),
        split_table(backward),
        split_table(last),
        twiddle,
    )


def halves(x):
    high = x.astype(BF16)
    return high, (x - high.astype(F32)).astype(BF16)


def dot(a, b):
    return jnp.dot(a, b, preferred_element_type=F32)


def table_dot(table, x, passes=3):
    if passes == 1:
        return dot(table[0], x.astype(BF16))
    high, low = halves(x)
    if passes == 2:
        return dot(table[0], high) + dot(table[0], low)
    return dot(table[0], high) + dot(table[0], low) + dot(table[1], high)


def dot_table(x, table, passes=3):
    if passes == 1:
        return dot(x.astype(BF16), table[0])
    high, low = halves(x)
    if passes == 2:
        return dot(high, table[0]) + dot(low, table[0])
    return dot(high, table[0]) + dot(low, table[0]) + dot(high, table[1])


def encode(early, base, taps_ref, offsets_ref, rates_ref):
    angles = rates_ref.shape[-1]
    empty = jnp.zeros((4, angles), F32)
    left = jnp.concatenate(
        [taps_ref[0, 0], taps_ref[0, 1], offsets_ref[0].astype(F32), rates_ref[0], empty], axis=0
    )
    for piece in range(3):
        high = left.astype(BF16)
        left = left - high.astype(F32)
        for at in range(angles // LANES):
            spot = base + 16 * (piece * (angles // LANES) + at)
            early[spot : spot + 16, :LANES] = high[:, at * LANES : (at + 1) * LANES]


def decode(ref, base, angles):
    pieces = []
    for piece in range(3):
        spots = [base + 16 * (piece * (angles // LANES) + at) for at in range(angles // LANES)]
        pieces.append(
            jnp.concatenate([ref[spot : spot + 16, :LANES] for spot in spots], axis=1).astype(F32)
        )
    return pieces[0] + pieces[1] + pieces[2]


def load_filter(raw_ref, filt_ref):
    radix = filt_ref.shape[1]
    period = math.lcm(radix, LANES)
    sections, rows = period // radix, period // LANES
    count = LANES // sections
    lane = lax.broadcasted_iota(jnp.int32, (count, LANES), 1)
    for part in range(2):
        near = [raw_ref[pl.ds(2 * o + part, count, stride=2 * rows), :] for o in range(rows)]
        stack = []
        for u in range(sections):
            at, skip = divmod(radix * u, LANES)
            cells = near[at]
            if skip:
                cells = pltpu.roll(cells, LANES - skip, 1)
                if skip + radix > LANES:
                    after = pltpu.roll(near[at + 1], LANES - skip, 1)
                    cells = jnp.where(lane < LANES - skip, cells, after)
            stack.append(cells)
        filt_ref[part] = jnp.transpose(jnp.concatenate(stack, axis=0))[:radix]


def compress_kernel(ranks, cuts, me_ref, shifts_ref, *refs):
    loads, outs = refs[:LOADS], refs[LOADS : LOADS + len(cuts) + 1]
    early = refs[LOADS + len(cuts) + 1]
    total, filt_ref, *held = refs[LOADS + len(cuts) + 2 : -1]
    done = refs[-1]
    echo_ref, first_ref, twiddle_ref, raw_ref, forward_ref, backward_ref, last_ref = held[:7]
    taps_ref, offsets_ref, rates_ref = held[7:]
    held = [*held, early.at[pl.ds(0, loads[-1].shape[0])]]

    def piece(step):
        cells = pl.ds(step * QUAD, QUAD)
        return pltpu.make_async_copy(
            loads[0].at[cells], echo_ref.at[cells], done.at[LOADS + step]
        )

    copies = [pltpu.make_async_copy(loads[i], held[i], done.at[i]) for i in range(1, LOADS)]
    copies[0].start()
    piece(0).start()
    for copy in copies[1:6]:
        copy.start()
    for step in range(1, echo_ref.shape[0] // QUAD):
        piece(step).start()
    for copy in copies[6:]:
        copy.start()
    copies[0].wait()
    pulses, radix = echo_ref.shape[0], echo_ref.shape[1] // 2
    wide = 2 * pulses
    me = me_ref[0]
    lane = lax.broadcasted_iota(jnp.int32, (radix, LANES), 1)
    row = lax.broadcasted_iota(jnp.int32, (radix, LANES), 0)
    sections = []
    for step in range(pulses // QUAD):
        piece(step).wait()
        x = jnp.concatenate([echo_ref[step * QUAD + q] for q in range(QUAD)], axis=1)
        y = table_dot(first_ref, x, PASSES[0])
        if not step:
            for copy in copies[1:6]:
                copy.wait()
            load_filter(raw_ref, filt_ref)
        for q in range(QUAD):
            here = slice(q * LANES, (q + 1) * LANES)
            turned = complex_times((y[:radix, here], y[radix:, here]), (twiddle_ref[0], -twiddle_ref[1]))
            sections.append(jnp.concatenate(turned, axis=1))
    z = dot_table(jnp.concatenate(sections, axis=0), forward_ref, PASSES[1])
    sections = []
    for q in range(pulses):
        here = slice(q * radix, (q + 1) * radix)
        turned = complex_times((z[here, :LANES], z[here, LANES:]), (filt_ref[0], filt_ref[1]))
        sections.append(jnp.concatenate(turned, axis=1))
    z = dot_table(jnp.concatenate(sections, axis=0), backward_ref, PASSES[2])
    sections = []
    for q in range(pulses):
        here = slice(q * radix, (q + 1) * radix)
        turned = complex_times((z[here, :LANES], z[here, LANES:]), (twiddle_ref[0], twiddle_ref[1]))
        sections.append(jnp.concatenate(turned, axis=0))
    y = table_dot(last_ref, jnp.concatenate(sections, axis=1), PASSES[3])
    for q in range(pulses):
        shift = shifts_ref[me * pulses + q]
        source = lane + shift
        for part in range(2):
            cells = y[part * radix : (part + 1) * radix, q * LANES : (q + 1) * LANES]
            turned = pltpu.roll(cells, lax.rem(LANES - shift, LANES), 1)
            after = jnp.where(row == radix - 1, 0.0, pltpu.roll(turned, radix - 1, 0))
            before = jnp.where(row == 0, 0.0, pltpu.roll(turned, 1, 0))
            moved = jnp.where(source >= LANES, after, jnp.where(source < 0, before, turned))
            total[pl.ds(part * pulses + q, radix, stride=wide), :] = moved

    for copy in copies[6:]:
        copy.wait()
    encode(early, loads[-1].shape[0], taps_ref, offsets_ref, rates_ref)
    length = radix // ranks * wide
    for d in range(ranks):
        start = pl.multiple_of(lax.bitwise_xor(me, d) * length, 8)
        if d % 2:
            outs[-1][d // 2] = total[pl.ds(start, length), :].astype(BF16)
            continue
        for cut, (low, high) in enumerate(cuts):
            cells = total[pl.ds(start + low * wide, (high - low) * wide), :]
            outs[cut][d // 2] = cells.astype(BF16)


def compress(echoes, filter_spectrum, range_shifts, steering, tap_offsets, tap_weights, phase_rates, me, ranks, cuts):
    pulses, _, samples = echoes.shape
    radix = samples // LANES
    wide = 2 * pulses
    view = echoes.reshape(pulses, 2, radix, LANES).transpose(0, 2, 1, 3)
    view = view.reshape(pulses, 2 * radix, LANES)
    filt = filter_spectrum.reshape(2, radix, LANES).transpose(1, 0, 2).reshape(2 * radix, LANES)
    angles = steering.shape[2]
    steer = steering.reshape(2 * angles, -1)
    first, forward, backward, last, twiddle = [jnp.asarray(t) for t in dft_tables(samples)]
    loads = [view, first, twiddle, filt, forward, backward, last]
    loads += [tap_weights, tap_offsets, phase_rates, steer]
    smem = pl.BlockSpec(memory_space=pltpu.SMEM)
    vmem = pl.BlockSpec(memory_space=pltpu.VMEM)
    away = pl.BlockSpec(memory_space=pltpu.HBM)
    half = ranks // 2
    return pl.pallas_call(
        functools.partial(compress_kernel, ranks, cuts),
        out_shape=[
            jax.ShapeDtypeStruct((half, (high - low) * wide, LANES), BF16)
            for low, high in [*cuts, (0, radix // ranks)]
        ]
        + [jax.ShapeDtypeStruct((2 * angles + 48 * angles // LANES, steer.shape[1]), BF16)],
        in_specs=[smem, smem] + [away] * LOADS,
        out_specs=[vmem] * (2 + len(cuts)),
        scratch_shapes=[pltpu.VMEM((radix * wide, LANES), F32), pltpu.VMEM((2, radix, LANES), F32)]
        + [pltpu.VMEM(x.shape, x.dtype) for x in loads[:-1]]
        + [pltpu.SemaphoreType.DMA((LOADS + pulses // QUAD,))],
        compiler_params=pltpu.CompilerParams(vmem_limit_bytes=COMPRESS_LIMIT),
        cost_estimate=pl.CostEstimate(
            flops=pulses * samples * 4000, bytes_accessed=pulses * samples * 12, transcendentals=0
        ),
        name="compress",
    )(me, range_shifts, *loads)


def pack_kernel(cuts, wide, *refs):
    near, far, outs = refs[: len(cuts)], refs[len(cuts)], refs[len(cuts) + 1 :]
    half = far.shape[0]
    for cut, (low, high) in enumerate(cuts):
        for z in range(half):
            outs[cut * half + z][0] = near[cut][z]
            outs[cut * half + z][1] = far[z, low * wide : high * wide]


def pack(near, far, cuts, wide):
    half = far.shape[0]
    vmem = pl.BlockSpec(memory_space=pltpu.VMEM)
    flat = pl.pallas_call(
        functools.partial(pack_kernel, cuts, wide),
        out_shape=[
            jax.ShapeDtypeStruct((2, (high - low) * wide, LANES), BF16)
            for low, high in cuts
            for _ in range(half)
        ],
        in_specs=[vmem] * (len(cuts) + 1),
        out_specs=[vmem] * (len(cuts) * half),
        compiler_params=pltpu.CompilerParams(vmem_limit_bytes=16 * 1024 * 1024),
        cost_estimate=pl.CostEstimate(flops=1 << 20, bytes_accessed=1 << 20, transcendentals=0),
        name="pack",
    )(*near, far)
    return [flat[cut * half : (cut + 1) * half] for cut in range(len(cuts))]


def twice(a):
    double = a[1] + a[1]
    return 1.0 - double * a[1], double * a[0]


def complex_times(a, b):
    return a[0] * b[0] - a[1] * b[1], a[0] * b[1] + a[1] * b[0]


def prepare_kernel(groups, ranks, rows, samples, pair, me_ref, *refs):
    steer = refs[:groups]
    mixes, mats, current, strides = refs[groups:]
    angles = mats.shape[-1]
    members = steer[0].shape[-1]
    me = me_ref[0]
    share = members // ranks
    column = lax.broadcasted_iota(jnp.int32, (members, 2 * members), 1)
    member = lax.broadcasted_iota(jnp.int32, (members, 2 * members), 0)
    slot = lax.div(column, 2 * share)
    within = lax.rem(column, 2 * share)
    part = lax.div(within, share)
    source = lax.bitwise_xor(slot, me) * share + lax.rem(within, share)
    picks = [
        jnp.where((part == c) & (source == member), 1.0, 0.0).astype(BF16) for c in range(2)
    ]
    below = lax.broadcasted_iota(jnp.int32, (angles, angles), 0)
    across = lax.broadcasted_iota(jnp.int32, (1, angles), 1)
    lane = lax.broadcasted_iota(jnp.int32, (angles, LANES), 1)
    small = lane.astype(F32) * (1.0 / samples)
    tables = [decode(steer[2 * pick], 2 * angles, angles) for pick in range(groups // 2)]
    rates = jnp.concatenate([table[10:12] for table in tables], axis=0)
    begin = rates * ((me * (rows * LANES)).astype(F32) * (1.0 / samples))
    lines = [rates, jnp.cos(begin), jnp.sin(begin)]
    for count in (1, pair):
        phase = rates * (count * LANES / samples)
        lines += [jnp.cos(phase), jnp.sin(phase)]
    lines.append(jnp.zeros((LANES - 7 * groups, angles), F32))
    lines = jnp.transpose(jnp.concatenate(lines, axis=0))

    def spread(kind, n):
        at = kind * groups + n
        return jnp.broadcast_to(lines[:, at : at + 1], (angles, LANES))

    for pick in range(groups // 2):
        offset = 2 * pick
        table = tables[pick]
        for h in range(2):
            moved = table[8 + h : 9 + h, :].astype(jnp.int32)
            total = jnp.zeros((angles, angles), F32)
            for tap in range(4):
                at_row = jnp.clip(across + moved + (tap - 1), 0, angles - 1)
                total = total + jnp.where(below == at_row, table[4 * h + tap : 4 * h + tap + 1, :], 0.0)
            matrix = jnp.transpose(total).astype(BF16)
            mats[2 * pick + h] = matrix
            near = steer[offset ^ h]
            real = dot(matrix, near[:angles, :]).astype(BF16)
            imag = dot(matrix, near[angles : 2 * angles, :]).astype(BF16)
            mixes[2 * pick + h, :angles, :] = (dot(real, picks[0]) - dot(imag, picks[1])).astype(BF16)
            mixes[2 * pick + h, angles:, :] = (dot(imag, picks[0]) + dot(real, picks[1])).astype(BF16)
            n = 2 * pick + h
            now = complex_times((spread(1, n), spread(2, n)), small_turn(spread(0, n) * small))
            current[n, 0, :, :LANES], current[n, 1, :, :LANES] = now
            if pair == 2:
                now = complex_times(now, (spread(3, n), spread(4, n)))
                current[n, 0, :, LANES:], current[n, 1, :, LANES:] = now
            strides[n, 0], strides[n, 1] = spread(5, n), spread(6, n)


def small_turn(x):
    y = x * x
    cosine = 1.0 - y * (0.5 - y * (1.0 / 24.0 - y * (1.0 / 720.0)))
    return cosine, x * (1.0 - y * (1.0 / 6.0 - y * (1.0 / 120.0 - y * (1.0 / 5040.0))))


def prepare(steer, angles, me, groups, ranks, rows, samples, pair):
    members = steer[0].shape[1]
    smem = pl.BlockSpec(memory_space=pltpu.SMEM)
    vmem = pl.BlockSpec(memory_space=pltpu.VMEM)
    return pl.pallas_call(
        functools.partial(prepare_kernel, groups, ranks, rows, samples, pair),
        out_shape=[
            jax.ShapeDtypeStruct((groups, 2 * angles, 2 * members), BF16),
            jax.ShapeDtypeStruct((groups, angles, angles), BF16),
            jax.ShapeDtypeStruct((groups, 2, angles, pair * LANES), F32),
            jax.ShapeDtypeStruct((groups, 2, angles, LANES), F32),
        ],
        in_specs=[smem] + [vmem] * len(steer),
        out_specs=[vmem] * 4,
        compiler_params=pltpu.CompilerParams(vmem_limit_bytes=32 * 1024 * 1024),
        cost_estimate=pl.CostEstimate(
            flops=groups * angles * members * 40000, bytes_accessed=8 << 20, transcendentals=0
        ),
        name="prepare",
    )(me, *steer)


BAND = 32


def merge_kernel(groups, layout, count, unit, mixes, mats, strides, start, *refs):
    levels = groups.bit_length() - 1
    parts = refs[: sum(len(p) for p in layout)]
    out, current, mixed, image, done = refs[-5:]
    held, at = [], 0
    for sizes in layout:
        held.append(parts[at : at + len(sizes)])
        at += len(sizes)
    if len(out.shape) == 3:
        out = out.reshape(out.shape[0] * out.shape[1], LANES)
    angles = mats.shape[-1]
    wide = held[0][0].shape[1] // count
    pair = 2 if unit % 2 == 0 else 1
    started = pl.program_id(0) * unit
    @pl.when(started == 0)
    def _():
        copy = pltpu.make_async_copy(start, current, done)
        copy.start()
        copy.wait()

    def column(offset, j):
        return jnp.concatenate(
            [
                ref[:, pl.ds(pl.multiple_of(j * wide, 8), wide), :].reshape(-1, LANES)
                for ref in held[offset]
            ],
            axis=0,
        )

    @pl.loop(0, unit // pair)
    def _(step):
        base = started + step * pair
        cells = [
            jnp.concatenate([column(offset, base + u) for u in range(pair)], axis=1)
            for offset in range(groups)
        ]
        for n in range(groups):
            pick, h = n // 2, n % 2
            mixed[n] = dot(mixes[n], cells[(2 * pick) ^ h])
        for level in range(levels):
            last = level == levels - 1
            stride = 2 << level
            if level:
                for offset in range(0, groups, stride):
                    for h in range(2):
                        n = offset + h
                        far = offset ^ (h << level)
                        mixed_out = dot(mats[n], image[far // 2])
                        mixed[n, :angles] = mixed_out[:, : pair * LANES]
                        mixed[n, angles:] = mixed_out[:, pair * LANES :]
            for offset in range(0, groups, stride):
                for top in range(0, angles, BAND):
                    band = slice(top, top + BAND)
                    lower = slice(angles + top, angles + top + BAND)
                    for u in range(pair):
                        here = slice(u * LANES, (u + 1) * LANES)
                        terms = []
                        for h in range(2):
                            n = offset + h
                            now = (current[n, 0, band, here], current[n, 1, band, here])
                            power = now
                            if level:
                                power = twice(now)
                            for _ in range(level - 1):
                                power = complex_times(power, now)
                            terms.append(
                                complex_times((mixed[n, band, here], mixed[n, lower, here]), power)
                            )
                            if last or offset % (2 * stride):
                                jump = (strides[n, 0, band], strides[n, 1, band])
                                moved = complex_times(now, jump)
                                current[n, 0, band, here], current[n, 1, band, here] = moved
                        re = terms[0][0] + terms[1][0]
                        im = terms[0][1] + terms[1][1]
                        if last:
                            spot = top * unit * 2 + (step * pair + u) * 2
                            out[pl.ds(spot, BAND, stride=unit * 2), :] = re
                            out[pl.ds(spot + 1, BAND, stride=unit * 2), :] = im
                        else:
                            image[offset // 2, band, here] = re.astype(BF16)
                            far_side = slice((pair + u) * LANES, (pair + u + 1) * LANES)
                            image[offset // 2, band, far_side] = im.astype(BF16)


def merge(held, mixes, mats, current, strides, rows, low, high, unit, before):
    groups, angles = mats.shape[0], mats.shape[-1]
    pair = 2 if unit % 2 == 0 else 1
    layout = [[part.shape[0] for part in parts] for parts in held]
    flat = [part for parts in held for part in parts]
    vmem = pl.BlockSpec(memory_space=pltpu.VMEM)
    if unit * 2 % 8:
        shape, block, spot = (angles * rows * 2, LANES), (angles * unit * 2, LANES), lambda i: (0, 0)
    else:
        shape, block = (angles, rows * 2, LANES), (angles, unit * 2, LANES)
        spot = lambda i: (0, low // unit + i, 0)
    operands = [mixes, mats, strides, current, *flat]
    specs = [vmem] * len(operands)
    aliases = {3: 1}
    if before is not None:
        aliases[len(operands)] = 0
        operands.append(before)
        specs.append(pl.BlockSpec(memory_space=pltpu.HBM))
    return pl.pallas_call(
        functools.partial(merge_kernel, groups, layout, high - low, unit),
        grid=((high - low) // unit,),
        out_shape=[jax.ShapeDtypeStruct(shape, F32), jax.ShapeDtypeStruct(current.shape, F32)],
        in_specs=specs,
        out_specs=[pl.BlockSpec(block, spot), vmem],
        input_output_aliases=aliases,
        scratch_shapes=[
            pltpu.VMEM((groups, 2 * angles, pair * LANES), F32),
            pltpu.VMEM((max(groups // 2, 1), angles, 2 * pair * LANES), BF16),
            pltpu.SemaphoreType.DMA,
        ],
        compiler_params=pltpu.CompilerParams(vmem_limit_bytes=VMEM_LIMIT),
        cost_estimate=pl.CostEstimate(
            flops=groups * angles * angles * (high - low) * LANES * 8,
            bytes_accessed=angles * (high - low) * LANES * 16,
            transcendentals=0,
        ),
        name="merge",
    )(*operands)


def hop(value, axis, offset):
    if not offset:
        return value
    return lax.ppermute(value, axis, [(i, i ^ offset) for i in range(lax.axis_size(axis))])


def neighbours(x, groups):
    return {1 << b: hop(x, "sub", 1 << b) for b in range(groups.bit_length() - 1)}


def others(x, near, groups):
    held = {0: [x]}
    for bit in near:
        held[bit] = [near[bit]]
    slots = x.shape[0]
    for offset in range(groups):
        if offset in held:
            continue
        via = [bit for bit in near if offset & bit]
        edges = [slots * i // len(via) for i in range(len(via) + 1)]
        pieces = []
        for bit, low, high in zip(via, edges[:-1], edges[1:]):
            source = held[offset ^ bit]
            source = source[0] if len(source) == 1 else jnp.concatenate(source, axis=0)
            pieces.append(hop(source[low:high], "sub", bit))
        held[offset] = pieces
    return [held[offset] for offset in range(groups)]


def local(echoes, filter_spectrum, range_shifts, steering, tap_offsets, tap_weights, phase_rates):
    ranks, groups = lax.axis_size("rng"), lax.axis_size("sub")
    pulses, _, samples = echoes.shape
    rows = samples // LANES // ranks
    angles = steering.shape[2]
    me = lax.axis_index("rng").astype(jnp.int32).reshape(1)
    unit = UNIT if rows % UNIT == 0 else rows
    edges = sorted({0, unit * (rows // unit * SHARE // 12), rows})
    cuts = list(zip(edges[:-1], edges[1:]))

    *near, odd, early = compress(
        echoes, filter_spectrum, range_shifts, steering, tap_offsets, tap_weights, phase_rates,
        me, ranks, cuts,
    )
    steers = [hop(early, "sub", e) for e in range(groups)]
    packed = pack(near, hop(odd, "rng", 1), cuts, 2 * pulses)
    arrived = [
        jnp.concatenate([hop(block, "rng", 2 * z) for z, block in enumerate(blocks)], axis=0)
        for blocks in packed
    ]
    nears = []
    for x in arrived:
        nears.append(neighbours(x, groups))
    steers, nears[0] = lax.optimization_barrier((steers, nears[0]))
    pair = 2 if unit % 2 == 0 else 1
    mixes, mats, current, strides = prepare(
        steers, angles, me, groups, ranks, rows, samples, pair
    )
    nears[-1], mixes = lax.optimization_barrier((nears[-1], mixes))
    out = None
    for cut, (low, high) in enumerate(cuts):
        held = others(arrived[cut], nears[cut], groups)
        out, current = merge(
            held, mixes, mats, current, strides, rows, low, high, unit, out
        )
    out = out.reshape(angles, rows, 2, LANES).transpose(0, 2, 1, 3)
    out = with_layout_constraint(out, Layout(major_to_minor=(0, 2, 1, 3)))
    return out.reshape(angles, 2, rows * LANES)


def solution(mesh):
    placed = (
        P(("sub", "rng"), None, None),
        P(),
        P("sub"),
        P("sub", None, None, None),
        P("sub", None, None),
        P("sub", None, None, None),
        P("sub", None, None),
    )
    return jax.shard_map(
        local, mesh=mesh, in_specs=placed, out_specs=P("sub", None, "rng"), check_vma=False
    )
```

```python
import functools
import math

import jax
import jax.numpy as jnp
import numpy as np
from jax import lax
from jax.experimental import pallas as pl
from jax.experimental.layout import Layout, with_layout_constraint
from jax.experimental.pallas import tpu as pltpu
from jax.sharding import PartitionSpec as P


LANES = 128
QUAD = 4
F32 = jnp.float32
BF16 = jnp.bfloat16
MERGE_LIMIT = 16 * 1024 * 1024
REACH = 6
UNIT = 4
SHARE = 4
LOADS = 11
PASSES = (3, 3, 1, 1)
COMPRESS_LIMIT = 60 * 1024 * 1024


def split_table(table):
    high = table.astype(np.float32).astype(BF16)
    low = (table - high.astype(np.float64)).astype(np.float32).astype(BF16)
    return np.stack([high, low])


def frequency_order(radix):
    sections = math.lcm(radix, LANES) // radix
    place = np.arange(LANES)
    return sections * (place % (LANES // sections)) + place // (LANES // sections)


@functools.lru_cache(None)
def dft_tables(samples):
    radix = samples // LANES
    outer = 2.0 * np.pi * (np.outer(np.arange(radix), np.arange(radix)) % radix) / radix
    inner = 2.0 * np.pi * (np.outer(np.arange(LANES), np.arange(LANES)) % LANES) / LANES
    turn = 2.0 * np.pi * np.outer(np.arange(radix), np.arange(LANES)) / samples
    c, s = np.cos(outer), np.sin(outer)
    first = np.concatenate(
        [np.stack([c, s], -1).reshape(radix, -1), np.stack([-s, c], -1).reshape(radix, -1)]
    )
    last = np.block([[c, -s], [s, c]]) / samples
    order = frequency_order(radix)
    c, s = np.cos(inner)[:, order], np.sin(inner)[:, order]
    forward = np.block([[c, -s], [s, c]])
    backward = np.block([[c.T, s.T], [-s.T, c.T]])
    twiddle = np.stack([np.cos(turn), np.sin(turn)]).astype(np.float32)
    return (
        split_table(first),
        split_table(forward),
        split_table(backward),
        split_table(last),
        twiddle,
    )


def halves(x):
    high = x.astype(BF16)
    return high, (x - high.astype(F32)).astype(BF16)


def dot(a, b):
    return jnp.dot(a, b, preferred_element_type=F32)


def table_dot(table, x, passes=3):
    if passes == 1:
        return dot(table[0], x.astype(BF16))
    high, low = halves(x)
    if passes == 2:
        return dot(table[0], high) + dot(table[0], low)
    return dot(table[0], high) + dot(table[0], low) + dot(table[1], high)


def dot_table(x, table, passes=3):
    if passes == 1:
        return dot(x.astype(BF16), table[0])
    high, low = halves(x)
    if passes == 2:
        return dot(high, table[0]) + dot(low, table[0])
    return dot(high, table[0]) + dot(low, table[0]) + dot(high, table[1])


def encode(early, base, taps_ref, offsets_ref, rates_ref):
    angles = rates_ref.shape[-1]
    empty = jnp.zeros((4, angles), F32)
    left = jnp.concatenate(
        [taps_ref[0, 0], taps_ref[0, 1], offsets_ref[0].astype(F32), rates_ref[0], empty], axis=0
    )
    for piece in range(3):
        high = left.astype(BF16)
        left = left - high.astype(F32)
        for at in range(angles // LANES):
            spot = base + 16 * (piece * (angles // LANES) + at)
            early[spot : spot + 16, :LANES] = high[:, at * LANES : (at + 1) * LANES]


def decode(ref, base, angles):
    pieces = []
    for piece in range(3):
        spots = [base + 16 * (piece * (angles // LANES) + at) for at in range(angles // LANES)]
        pieces.append(
            jnp.concatenate([ref[spot : spot + 16, :LANES] for spot in spots], axis=1).astype(F32)
        )
    return pieces[0] + pieces[1] + pieces[2]


def load_filter(raw_ref, filt_ref):
    radix = filt_ref.shape[1]
    period = math.lcm(radix, LANES)
    sections, rows = period // radix, period // LANES
    count = LANES // sections
    lane = lax.broadcasted_iota(jnp.int32, (count, LANES), 1)
    for part in range(2):
        near = [raw_ref[pl.ds(2 * o + part, count, stride=2 * rows), :] for o in range(rows)]
        stack = []
        for u in range(sections):
            at, skip = divmod(radix * u, LANES)
            cells = near[at]
            if skip:
                cells = pltpu.roll(cells, LANES - skip, 1)
                if skip + radix > LANES:
                    after = pltpu.roll(near[at + 1], LANES - skip, 1)
                    cells = jnp.where(lane < LANES - skip, cells, after)
            stack.append(cells)
        filt_ref[part] = jnp.transpose(jnp.concatenate(stack, axis=0))[:radix]


def compress_kernel(ranks, cuts, me_ref, shifts_ref, *refs):
    loads, outs = refs[:LOADS], refs[LOADS : LOADS + len(cuts) + 1]
    early = refs[LOADS + len(cuts) + 1]
    total, filt_ref, *held = refs[LOADS + len(cuts) + 2 : -1]
    done = refs[-1]
    echo_ref, first_ref, twiddle_ref, raw_ref, forward_ref, backward_ref, last_ref = held[:7]
    taps_ref, offsets_ref, rates_ref = held[7:]
    held = [*held, early.at[pl.ds(0, loads[-1].shape[0])]]

    def piece(step):
        cells = pl.ds(step * QUAD, QUAD)
        return pltpu.make_async_copy(
            loads[0].at[cells], echo_ref.at[cells], done.at[LOADS + step]
        )

    copies = [pltpu.make_async_copy(loads[i], held[i], done.at[i]) for i in range(1, LOADS)]
    copies[0].start()
    piece(0).start()
    for copy in copies[1:6]:
        copy.start()
    for step in range(1, echo_ref.shape[0] // QUAD):
        piece(step).start()
    for copy in copies[6:]:
        copy.start()
    copies[0].wait()
    pulses, radix = echo_ref.shape[0], echo_ref.shape[1] // 2
    wide = 2 * pulses
    me = me_ref[0]
    lane = lax.broadcasted_iota(jnp.int32, (radix, LANES), 1)
    row = lax.broadcasted_iota(jnp.int32, (radix, LANES), 0)
    sections = []
    for step in range(pulses // QUAD):
        piece(step).wait()
        x = jnp.concatenate([echo_ref[step * QUAD + q] for q in range(QUAD)], axis=1)
        y = table_dot(first_ref, x, PASSES[0])
        if not step:
            for copy in copies[1:6]:
                copy.wait()
            load_filter(raw_ref, filt_ref)
        for q in range(QUAD):
            here = slice(q * LANES, (q + 1) * LANES)
            turned = complex_times((y[:radix, here], y[radix:, here]), (twiddle_ref[0], -twiddle_ref[1]))
            sections.append(jnp.concatenate(turned, axis=1))
    z = dot_table(jnp.concatenate(sections, axis=0), forward_ref, PASSES[1])
    sections = []
    for q in range(pulses):
        here = slice(q * radix, (q + 1) * radix)
        turned = complex_times((z[here, :LANES], z[here, LANES:]), (filt_ref[0], filt_ref[1]))
        sections.append(jnp.concatenate(turned, axis=1))
    z = dot_table(jnp.concatenate(sections, axis=0), backward_ref, PASSES[2])
    sections = []
    for q in range(pulses):
        here = slice(q * radix, (q + 1) * radix)
        turned = complex_times((z[here, :LANES], z[here, LANES:]), (twiddle_ref[0], twiddle_ref[1]))
        sections.append(jnp.concatenate(turned, axis=0))
    y = table_dot(last_ref, jnp.concatenate(sections, axis=1), PASSES[3])
    for q in range(pulses):
        shift = shifts_ref[me * pulses + q]
        source = lane + shift
        for part in range(2):
            cells = y[part * radix : (part + 1) * radix, q * LANES : (q + 1) * LANES]
            turned = pltpu.roll(cells, lax.rem(LANES - shift, LANES), 1)
            after = jnp.where(row == radix - 1, 0.0, pltpu.roll(turned, radix - 1, 0))
            before = jnp.where(row == 0, 0.0, pltpu.roll(turned, 1, 0))
            moved = jnp.where(source >= LANES, after, jnp.where(source < 0, before, turned))
            total[pl.ds(part * pulses + q, radix, stride=wide), :] = moved

    for copy in copies[6:]:
        copy.wait()
    encode(early, loads[-1].shape[0], taps_ref, offsets_ref, rates_ref)
    length = radix // ranks * wide
    for d in range(ranks):
        start = pl.multiple_of(lax.bitwise_xor(me, d) * length, 8)
        if d % 2:
            outs[-1][d // 2] = total[pl.ds(start, length), :].astype(BF16)
            continue
        for cut, (low, high) in enumerate(cuts):
            cells = total[pl.ds(start + low * wide, (high - low) * wide), :]
            outs[cut][d // 2] = cells.astype(BF16)


def compress(echoes, filter_spectrum, range_shifts, steering, tap_offsets, tap_weights, phase_rates, me, ranks, cuts):
    pulses, _, samples = echoes.shape
    radix = samples // LANES
    wide = 2 * pulses
    view = echoes.reshape(pulses, 2, radix, LANES).transpose(0, 2, 1, 3)
    view = view.reshape(pulses, 2 * radix, LANES)
    filt = filter_spectrum.reshape(2, radix, LANES).transpose(1, 0, 2).reshape(2 * radix, LANES)
    angles = steering.shape[2]
    steer = steering.reshape(2 * angles, -1)
    first, forward, backward, last, twiddle = [jnp.asarray(t) for t in dft_tables(samples)]
    loads = [view, first, twiddle, filt, forward, backward, last]
    loads += [tap_weights, tap_offsets, phase_rates, steer]
    smem = pl.BlockSpec(memory_space=pltpu.SMEM)
    vmem = pl.BlockSpec(memory_space=pltpu.VMEM)
    away = pl.BlockSpec(memory_space=pltpu.HBM)
    half = ranks // 2
    return pl.pallas_call(
        functools.partial(compress_kernel, ranks, cuts),
        out_shape=[
            jax.ShapeDtypeStruct((half, (high - low) * wide, LANES), BF16)
            for low, high in [*cuts, (0, radix // ranks)]
        ]
        + [jax.ShapeDtypeStruct((2 * angles + 48 * angles // LANES, steer.shape[1]), BF16)],
        in_specs=[smem, smem] + [away] * LOADS,
        out_specs=[vmem] * (2 + len(cuts)),
        scratch_shapes=[pltpu.VMEM((radix * wide, LANES), F32), pltpu.VMEM((2, radix, LANES), F32)]
        + [pltpu.VMEM(x.shape, x.dtype) for x in loads[:-1]]
        + [pltpu.SemaphoreType.DMA((LOADS + pulses // QUAD,))],
        compiler_params=pltpu.CompilerParams(vmem_limit_bytes=COMPRESS_LIMIT),
        cost_estimate=pl.CostEstimate(
            flops=pulses * samples * 4000, bytes_accessed=pulses * samples * 12, transcendentals=0
        ),
        name="compress",
    )(me, range_shifts, *loads)


def pack_kernel(cuts, wide, *refs):
    near, far, outs = refs[: len(cuts)], refs[len(cuts)], refs[len(cuts) + 1 :]
    half = far.shape[0]
    for cut, (low, high) in enumerate(cuts):
        for z in range(half):
            outs[cut * half + z][0] = near[cut][z]
            outs[cut * half + z][1] = far[z, low * wide : high * wide]


def pack(near, far, cuts, wide):
    half = far.shape[0]
    vmem = pl.BlockSpec(memory_space=pltpu.VMEM)
    flat = pl.pallas_call(
        functools.partial(pack_kernel, cuts, wide),
        out_shape=[
            jax.ShapeDtypeStruct((2, (high - low) * wide, LANES), BF16)
            for low, high in cuts
            for _ in range(half)
        ],
        in_specs=[vmem] * (len(cuts) + 1),
        out_specs=[vmem] * (len(cuts) * half),
        compiler_params=pltpu.CompilerParams(vmem_limit_bytes=16 * 1024 * 1024),
        cost_estimate=pl.CostEstimate(flops=1 << 20, bytes_accessed=1 << 20, transcendentals=0),
        name="pack",
    )(*near, far)
    return [flat[cut * half : (cut + 1) * half] for cut in range(len(cuts))]


def twice(a):
    double = a[1] + a[1]
    return 1.0 - double * a[1], double * a[0]


def complex_times(a, b):
    return a[0] * b[0] - a[1] * b[1], a[0] * b[1] + a[1] * b[0]


def prepare_kernel(groups, ranks, rows, samples, pair, cuts, me_ref, *refs):
    steer = refs[:groups]
    mixes, mats, *turns = refs[groups:]
    places = [(cut, at) for cut, (low, high) in enumerate(cuts) for at in range((high - low) // pair)]
    angles = mats.shape[-1]
    members = steer[0].shape[-1]
    me = me_ref[0]
    share = members // ranks
    column = lax.broadcasted_iota(jnp.int32, (members, 2 * members), 1)
    member = lax.broadcasted_iota(jnp.int32, (members, 2 * members), 0)
    slot = lax.div(column, 2 * share)
    within = lax.rem(column, 2 * share)
    part = lax.div(within, share)
    source = lax.bitwise_xor(slot, me) * share + lax.rem(within, share)
    picks = [
        jnp.where((part == c) & (source == member), 1.0, 0.0).astype(BF16) for c in range(2)
    ]
    below = lax.broadcasted_iota(jnp.int32, (angles, angles), 0)
    across = lax.broadcasted_iota(jnp.int32, (1, angles), 1)
    lane = lax.broadcasted_iota(jnp.int32, (angles, LANES), 1)
    small = lane.astype(F32) * (1.0 / samples)
    tables = [decode(steer[2 * pick], 2 * angles, angles) for pick in range(groups // 2)]
    rates = jnp.concatenate([table[10:12] for table in tables], axis=0)
    begin = rates * ((me * (rows * LANES)).astype(F32) * (1.0 / samples))
    lines = [rates, jnp.cos(begin), jnp.sin(begin)]
    for count in (1, pair):
        phase = rates * (count * LANES / samples)
        lines += [jnp.cos(phase), jnp.sin(phase)]
    lines.append(jnp.zeros((LANES - 7 * groups, angles), F32))
    lines = jnp.transpose(jnp.concatenate(lines, axis=0))

    def spread(kind, n):
        at = kind * groups + n
        return jnp.broadcast_to(lines[:, at : at + 1], (angles, LANES))

    for pick in range(groups // 2):
        offset = 2 * pick
        table = tables[pick]
        for h in range(2):
            moved = table[8 + h : 9 + h, :].astype(jnp.int32)
            total = jnp.zeros((angles, angles), F32)
            for tap in range(4):
                at_row = jnp.clip(across + moved + (tap - 1), 0, angles - 1)
                total = total + jnp.where(below == at_row, table[4 * h + tap : 4 * h + tap + 1, :], 0.0)
            matrix = jnp.transpose(total).astype(BF16)
            mats[2 * pick + h] = matrix
            near = steer[offset ^ h]
            real = dot(matrix, near[:angles, :]).astype(BF16)
            imag = dot(matrix, near[angles : 2 * angles, :]).astype(BF16)
            mixes[2 * pick + h, :angles, :] = (dot(real, picks[0]) - dot(imag, picks[1])).astype(BF16)
            mixes[2 * pick + h, angles:, :] = (dot(imag, picks[0]) + dot(real, picks[1])).astype(BF16)
            n = 2 * pick + h
            now = complex_times((spread(1, n), spread(2, n)), small_turn(spread(0, n) * small))
            first = now
            step = (spread(3, n), spread(4, n))
            for u in range(pair):
                here = slice(u * LANES, (u + 1) * LANES)
                if u:
                    first = complex_times(first, step)
                now = first
                jump = (spread(5, n), spread(6, n))
                for index, (cut, at) in enumerate(places):
                    if index:
                        now = complex_times(now, jump)
                    turns[cut][at, n, 0, :, here], turns[cut][at, n, 1, :, here] = now


def small_turn(x):
    y = x * x
    cosine = 1.0 - y * (0.5 - y * (1.0 / 24.0 - y * (1.0 / 720.0)))
    return cosine, x * (1.0 - y * (1.0 / 6.0 - y * (1.0 / 120.0 - y * (1.0 / 5040.0))))


def prepare(steer, angles, me, groups, ranks, rows, samples, pair, cuts):
    members = steer[0].shape[1]
    smem = pl.BlockSpec(memory_space=pltpu.SMEM)
    vmem = pl.BlockSpec(memory_space=pltpu.VMEM)
    return pl.pallas_call(
        functools.partial(prepare_kernel, groups, ranks, rows, samples, pair, cuts),
        out_shape=[
            jax.ShapeDtypeStruct((groups, 2 * angles, 2 * members), BF16),
            jax.ShapeDtypeStruct((groups, angles, angles), BF16),
        ]
        + [
            jax.ShapeDtypeStruct(((high - low) // pair, groups, 2, angles, pair * LANES), F32)
            for low, high in cuts
        ],
        in_specs=[smem] + [vmem] * len(steer),
        out_specs=[vmem] * (2 + len(cuts)),
        compiler_params=pltpu.CompilerParams(vmem_limit_bytes=32 * 1024 * 1024),
        cost_estimate=pl.CostEstimate(
            flops=groups * angles * members * 40000, bytes_accessed=8 << 20, transcendentals=0
        ),
        name="prepare",
    )(me, *steer)


BAND = 32


def direct(source):
    return source & (source - 1) == 0


def kinds(groups):
    whole = [p for p in range(groups // 2) if direct(2 * p) and direct(2 * p + 1)]
    half = [p for p in range(groups // 2) if direct(2 * p) and not direct(2 * p + 1)]
    return whole, half


def columns(parts, wide, base, pair):
    return jnp.concatenate(
        [
            jnp.concatenate(
                [
                    ref[:, pl.ds(pl.multiple_of((base + u) * wide, 8), wide), :].reshape(-1, LANES)
                    for ref in parts
                ],
                axis=0,
            )
            for u in range(pair)
        ],
        axis=1,
    )


def rotated(mixed, turns, at, n, level, top, angles):
    band = slice(top, top + BAND)
    lower = slice(angles + top, angles + top + BAND)
    now = (turns[at, n, 0, band], turns[at, n, 1, band])
    power = twice(now) if level else now
    for _ in range(level - 1):
        power = complex_times(power, now)
    return complex_times((mixed[n, band], mixed[n, lower]), power)


def add(a, b):
    return a[0] + b[0], a[1] + b[1]


def near_kernel(groups, count, layout, mixes, turns, *refs):
    image, partial, mixed = refs[-3:]
    held = split(refs[:-3], layout)
    whole, half = kinds(groups)
    pair, angles = turns.shape[-1] // LANES, turns.shape[-2]
    wide = held[0][0].shape[1] // (count * pair)

    @pl.loop(0, count)
    def _(step):
        here = step
        cells = {o: columns(parts, wide, step * pair, pair) for o, parts in held.items()}
        ready = [n for n in range(groups) if direct(n)]
        for n in ready:
            mixed[n] = dot(mixes[n], cells[n])
        for pick in range(groups // 2):
            terms = [n for n in (2 * pick, 2 * pick + 1) if n in ready]
            for top in range(0, angles if terms else 0, BAND):
                band = slice(top, top + BAND)
                total = rotated(mixed, turns, here, terms[0], 0, top, angles)
                if len(terms) == 2:
                    total = add(total, rotated(mixed, turns, here, terms[1], 0, top, angles))
                    side = pair * LANES
                    image[step, whole.index(pick), band, :side] = total[0].astype(BF16)
                    image[step, whole.index(pick), band, side:] = total[1].astype(BF16)
                else:
                    spot = half.index(pick)
                    partial[step, spot, 0, band], partial[step, spot, 1, band] = total


def far_kernel(groups, count, layout, unit, mixes, mats, turns, image, partial, *refs):
    out, mixed, images = refs[-3:]
    held = split(refs[: sum(len(parts) for parts in layout.values())], layout)
    levels = groups.bit_length() - 1
    whole, half = kinds(groups)
    pair, angles = turns.shape[-1] // LANES, turns.shape[-2]
    wide = held[groups - 1][0].shape[1] // (count * pair)
    side = pair * LANES
    started = pl.program_id(0) * (unit // pair)
    middle = angles // 2
    window = min(angles, -(-(middle + REACH) // LANES) * LANES)
    if len(out.shape) == 3:
        out = out.reshape(out.shape[0] * out.shape[1], LANES)

    @pl.loop(0, unit // pair)
    def _(step):
        place = started + step
        here = place
        cells = {o: columns(parts, wide, place * pair, pair) for o, parts in held.items()}
        late = [n for n in range(groups) if n in held]
        for n in late:
            mixed[n] = dot(mixes[n], cells[n])
        for pick in range(groups // 2):
            terms = [n for n in (2 * pick, 2 * pick + 1) if n in late]
            if not terms:
                images[pick] = image[place, whole.index(pick)]
                continue
            for top in range(0, angles, BAND):
                band = slice(top, top + BAND)
                total = rotated(mixed, turns, here, terms[0], 0, top, angles)
                if len(terms) == 2:
                    total = add(total, rotated(mixed, turns, here, terms[1], 0, top, angles))
                else:
                    spot = half.index(pick)
                    total = add(total, (partial[place, spot, 0, band], partial[place, spot, 1, band]))
                images[pick, band, :side] = total[0].astype(BF16)
                images[pick, band, side:] = total[1].astype(BF16)
        for level in range(1, levels):
            last = level == levels - 1
            stride = 2 << level
            for offset in range(0, groups, stride):
                for h in range(2):
                    n = offset + h
                    source = images.at[(offset ^ (h << level)) // 2]
                    for low, high, start in ((0, middle, 0), (middle, angles, angles - window)):
                        turned = dot(mats[n, low:high, start : start + window], source[start : start + window])
                        mixed[n, low:high] = turned[:, :side]
                        mixed[n, angles + low : angles + high] = turned[:, side:]
            for offset in range(0, groups, stride):
                for top in range(0, angles, BAND):
                    band = slice(top, top + BAND)
                    re, im = add(
                        rotated(mixed, turns, here, offset, level, top, angles),
                        rotated(mixed, turns, here, offset + 1, level, top, angles),
                    )
                    if not last:
                        images[offset // 2, band, :side] = re.astype(BF16)
                        images[offset // 2, band, side:] = im.astype(BF16)
                        continue
                    for u in range(pair):
                        lanes = slice(u * LANES, (u + 1) * LANES)
                        spot = top * unit * 2 + (step * pair + u) * 2
                        out[pl.ds(spot, BAND, stride=unit * 2), :] = re[:, lanes]
                        out[pl.ds(spot + 1, BAND, stride=unit * 2), :] = im[:, lanes]


def split(refs, layout):
    held, at = {}, 0
    for offset, parts in layout.items():
        held[offset] = refs[at : at + len(parts)]
        at += len(parts)
    return held


def merge_near(held, mixes, turns, low, high):
    groups, pair, angles = mixes.shape[0], turns.shape[-1] // LANES, turns.shape[-2]
    vmem = pl.BlockSpec(memory_space=pltpu.VMEM)
    count = (high - low) // pair
    whole, half = kinds(groups)
    flat = [part for parts in held.values() for part in parts]
    return pl.pallas_call(
        functools.partial(near_kernel, groups, count, held),
        out_shape=[
            jax.ShapeDtypeStruct((count, len(whole), angles, 2 * pair * LANES), BF16),
            jax.ShapeDtypeStruct((count, len(half), 2, angles, pair * LANES), F32),
        ],
        in_specs=[vmem] * (2 + len(flat)),
        out_specs=[vmem] * 2,
        scratch_shapes=[pltpu.VMEM((groups, 2 * angles, pair * LANES), F32)],
        compiler_params=pltpu.CompilerParams(vmem_limit_bytes=MERGE_LIMIT),
        cost_estimate=pl.CostEstimate(
            flops=groups * angles * angles * (high - low) * LANES * 4,
            bytes_accessed=angles * (high - low) * LANES * 8,
            transcendentals=0,
        ),
        name="merge_near",
    )(mixes, turns, *flat)


def merge_far(held, mixes, mats, turns, image, partial, rows, low, high, unit, before):
    groups, pair, angles = mixes.shape[0], turns.shape[-1] // LANES, turns.shape[-2]
    vmem = pl.BlockSpec(memory_space=pltpu.VMEM)
    flat = [part for parts in held.values() for part in parts]
    if unit * 2 % 8:
        shape, block, spot = (angles * rows * 2, LANES), (angles * unit * 2, LANES), lambda i: (0, 0)
    else:
        shape, block = (angles, rows * 2, LANES), (angles, unit * 2, LANES)
        spot = lambda i: (0, low // unit + i, 0)
    operands = [mixes, mats, turns, image, partial, *flat]
    specs = [vmem] * len(operands)
    aliases = {}
    if before is not None:
        aliases[len(operands)] = 0
        operands.append(before)
        specs.append(pl.BlockSpec(memory_space=pltpu.HBM))
    return pl.pallas_call(
        functools.partial(far_kernel, groups, (high - low) // pair, held, unit),
        grid=((high - low) // unit,),
        out_shape=jax.ShapeDtypeStruct(shape, F32),
        in_specs=specs,
        out_specs=pl.BlockSpec(block, spot),
        input_output_aliases=aliases,
        scratch_shapes=[
            pltpu.VMEM((groups, 2 * angles, pair * LANES), F32),
            pltpu.VMEM((groups // 2, angles, 2 * pair * LANES), BF16),
        ],
        compiler_params=pltpu.CompilerParams(vmem_limit_bytes=MERGE_LIMIT),
        cost_estimate=pl.CostEstimate(
            flops=groups * angles * angles * (high - low) * LANES * 4,
            bytes_accessed=angles * (high - low) * LANES * 16,
            transcendentals=0,
        ),
        name="merge_far",
    )(*operands)


def hop(value, axis, offset):
    if not offset:
        return value
    return lax.ppermute(value, axis, [(i, i ^ offset) for i in range(lax.axis_size(axis))])


def neighbours(x, groups):
    return {1 << b: hop(x, "sub", 1 << b) for b in range(groups.bit_length() - 1)}


def others(x, near, groups):
    held = {0: [x]}
    for bit in near:
        held[bit] = [near[bit]]
    slots = x.shape[0]
    for offset in range(groups):
        if offset in held:
            continue
        via = [bit for bit in near if offset & bit]
        edges = [slots * i // len(via) for i in range(len(via) + 1)]
        pieces = []
        for bit, low, high in zip(via, edges[:-1], edges[1:]):
            source = held[offset ^ bit]
            source = source[0] if len(source) == 1 else jnp.concatenate(source, axis=0)
            pieces.append(hop(source[low:high], "sub", bit))
        held[offset] = pieces
    return [held[offset] for offset in range(groups)]


def local(echoes, filter_spectrum, range_shifts, steering, tap_offsets, tap_weights, phase_rates):
    ranks, groups = lax.axis_size("rng"), lax.axis_size("sub")
    pulses, _, samples = echoes.shape
    rows = samples // LANES // ranks
    angles = steering.shape[2]
    me = lax.axis_index("rng").astype(jnp.int32).reshape(1)
    unit = UNIT if rows % UNIT == 0 else rows
    edges = sorted({0, unit * (rows // unit * SHARE // 12), rows})
    cuts = list(zip(edges[:-1], edges[1:]))

    *near, odd, early = compress(
        echoes, filter_spectrum, range_shifts, steering, tap_offsets, tap_weights, phase_rates,
        me, ranks, cuts,
    )
    steers = [hop(early, "sub", e) for e in range(groups)]
    packed = pack(near, hop(odd, "rng", 1), cuts, 2 * pulses)
    arrived = [
        jnp.concatenate([hop(block, "rng", 2 * z) for z, block in enumerate(blocks)], axis=0)
        for blocks in packed
    ]
    nears = []
    for x in arrived:
        nears.append(neighbours(x, groups))
    steers, nears[0] = lax.optimization_barrier((steers, nears[0]))
    pair = 2 if unit % 2 == 0 else 1
    mixes, mats, *turns = prepare(steers, angles, me, groups, ranks, rows, samples, pair, cuts)
    out = None
    for cut, (low, high) in enumerate(cuts):
        held = others(arrived[cut], nears[cut], groups)
        close = {o: held[o] for o in range(groups) if direct(o)}
        far = {o: held[o] for o in range(groups) if not direct(o)}
        image, partial = merge_near(close, mixes, turns[cut], low, high)
        out = merge_far(far, mixes, mats, turns[cut], image, partial, rows, low, high, unit, out)
        if cut + 1 < len(cuts):
            nears[cut + 1], image = lax.optimization_barrier((nears[cut + 1], image))
    out = out.reshape(angles, rows, 2, LANES).transpose(0, 2, 1, 3)
    out = with_layout_constraint(out, Layout(major_to_minor=(0, 2, 1, 3)))
    return out.reshape(angles, 2, rows * LANES)


def solution(mesh):
    placed = (
        P(("sub", "rng"), None, None),
        P(),
        P("sub"),
        P("sub", None, None, None),
        P("sub", None, None),
        P("sub", None, None, None),
        P("sub", None, None),
    )
    return jax.shard_map(
        local, mesh=mesh, in_specs=placed, out_specs=P("sub", None, "rng"), check_vma=False
    )
```

```python
import functools
import math

import jax
import jax.numpy as jnp
import numpy as np
from jax import lax
from jax.experimental import pallas as pl
from jax.experimental.layout import Layout, with_layout_constraint
from jax.experimental.pallas import tpu as pltpu
from jax.sharding import PartitionSpec as P


LANES = 128
QUAD = 4
F32 = jnp.float32
BF16 = jnp.bfloat16
MERGE_LIMIT = 16 * 1024 * 1024
REACH = 6
UNIT = 4
LOADS = 11
PASSES = (3, 3, 1, 1)
COMPRESS_LIMIT = 60 * 1024 * 1024


def split_table(table):
    high = table.astype(np.float32).astype(BF16)
    low = (table - high.astype(np.float64)).astype(np.float32).astype(BF16)
    return np.stack([high, low])


def frequency_order(radix):
    sections = math.lcm(radix, LANES) // radix
    place = np.arange(LANES)
    return sections * (place % (LANES // sections)) + place // (LANES // sections)


@functools.lru_cache(None)
def dft_tables(samples):
    radix = samples // LANES
    outer = 2.0 * np.pi * (np.outer(np.arange(radix), np.arange(radix)) % radix) / radix
    inner = 2.0 * np.pi * (np.outer(np.arange(LANES), np.arange(LANES)) % LANES) / LANES
    turn = 2.0 * np.pi * np.outer(np.arange(radix), np.arange(LANES)) / samples
    c, s = np.cos(outer), np.sin(outer)
    first = np.concatenate(
        [np.stack([c, s], -1).reshape(radix, -1), np.stack([-s, c], -1).reshape(radix, -1)]
    )
    last = np.block([[c, -s], [s, c]]) / samples
    order = frequency_order(radix)
    c, s = np.cos(inner)[:, order], np.sin(inner)[:, order]
    forward = np.block([[c, -s], [s, c]])
    backward = np.block([[c.T, s.T], [-s.T, c.T]])
    twiddle = np.stack([np.cos(turn), np.sin(turn)]).astype(np.float32)
    return (
        split_table(first),
        split_table(forward),
        split_table(backward),
        split_table(last),
        twiddle,
    )


def halves(x):
    high = x.astype(BF16)
    return high, (x - high.astype(F32)).astype(BF16)


def dot(a, b):
    return jnp.dot(a, b, preferred_element_type=F32)


def table_dot(table, x, passes=3):
    if passes == 1:
        return dot(table[0], x.astype(BF16))
    high, low = halves(x)
    if passes == 2:
        return dot(table[0], high) + dot(table[0], low)
    return dot(table[0], high) + dot(table[0], low) + dot(table[1], high)


def dot_table(x, table, passes=3):
    if passes == 1:
        return dot(x.astype(BF16), table[0])
    high, low = halves(x)
    if passes == 2:
        return dot(high, table[0]) + dot(low, table[0])
    return dot(high, table[0]) + dot(low, table[0]) + dot(high, table[1])


def encode(early, base, taps_ref, offsets_ref, rates_ref):
    angles = rates_ref.shape[-1]
    empty = jnp.zeros((4, angles), F32)
    left = jnp.concatenate(
        [taps_ref[0, 0], taps_ref[0, 1], offsets_ref[0].astype(F32), rates_ref[0], empty], axis=0
    )
    for piece in range(3):
        high = left.astype(BF16)
        left = left - high.astype(F32)
        for at in range(angles // LANES):
            spot = base + 16 * (piece * (angles // LANES) + at)
            early[spot : spot + 16, :LANES] = high[:, at * LANES : (at + 1) * LANES]


def decode(ref, base, angles):
    pieces = []
    for piece in range(3):
        spots = [base + 16 * (piece * (angles // LANES) + at) for at in range(angles // LANES)]
        pieces.append(
            jnp.concatenate([ref[spot : spot + 16, :LANES] for spot in spots], axis=1).astype(F32)
        )
    return pieces[0] + pieces[1] + pieces[2]


def load_filter(raw_ref, filt_ref):
    radix = filt_ref.shape[1]
    period = math.lcm(radix, LANES)
    sections, rows = period // radix, period // LANES
    count = LANES // sections
    lane = lax.broadcasted_iota(jnp.int32, (count, LANES), 1)
    for part in range(2):
        near = [raw_ref[pl.ds(2 * o + part, count, stride=2 * rows), :] for o in range(rows)]
        stack = []
        for u in range(sections):
            at, skip = divmod(radix * u, LANES)
            cells = near[at]
            if skip:
                cells = pltpu.roll(cells, LANES - skip, 1)
                if skip + radix > LANES:
                    after = pltpu.roll(near[at + 1], LANES - skip, 1)
                    cells = jnp.where(lane < LANES - skip, cells, after)
            stack.append(cells)
        filt_ref[part] = jnp.transpose(jnp.concatenate(stack, axis=0))[:radix]


def compress_kernel(ranks, me_ref, shifts_ref, *refs):
    loads, (near, odd, early) = refs[:LOADS], refs[LOADS : LOADS + 3]
    total, filt_ref, *held = refs[LOADS + 3 : -1]
    done = refs[-1]
    echo_ref, first_ref, twiddle_ref, raw_ref, forward_ref, backward_ref, last_ref = held[:7]
    taps_ref, offsets_ref, rates_ref = held[7:]
    held = [*held, early.at[pl.ds(0, loads[-1].shape[0])]]

    def piece(step):
        cells = pl.ds(step * QUAD, QUAD)
        return pltpu.make_async_copy(
            loads[0].at[cells], echo_ref.at[cells], done.at[LOADS + step]
        )

    copies = [pltpu.make_async_copy(loads[i], held[i], done.at[i]) for i in range(1, LOADS)]
    first, twiddle, raw, forward, backward, last = copies[:6]
    first.start()
    piece(0).start()
    twiddle.start()
    for step in range(1, echo_ref.shape[0] // QUAD):
        piece(step).start()
    for copy in (*copies[6:], raw, forward, backward, last):
        copy.start()
    first.wait()
    pulses, radix = echo_ref.shape[0], echo_ref.shape[1] // 2
    wide = 2 * pulses
    me = me_ref[0]
    lane = lax.broadcasted_iota(jnp.int32, (radix, LANES), 1)
    row = lax.broadcasted_iota(jnp.int32, (radix, LANES), 0)
    sections = []
    for step in range(pulses // QUAD):
        piece(step).wait()
        x = jnp.concatenate([echo_ref[step * QUAD + q] for q in range(QUAD)], axis=1)
        y = table_dot(first_ref, x, PASSES[0])
        if not step:
            twiddle.wait()
        for q in range(QUAD):
            here = slice(q * LANES, (q + 1) * LANES)
            turned = complex_times((y[:radix, here], y[radix:, here]), (twiddle_ref[0], -twiddle_ref[1]))
            sections.append(jnp.concatenate(turned, axis=1))
    for copy in (*copies[6:], raw, forward, backward, last):
        copy.wait()
    load_filter(raw_ref, filt_ref)
    encode(early, loads[-1].shape[0], taps_ref, offsets_ref, rates_ref)
    z = dot_table(jnp.concatenate(sections, axis=0), forward_ref, PASSES[1])
    sections = []
    for q in range(pulses):
        here = slice(q * radix, (q + 1) * radix)
        turned = complex_times((z[here, :LANES], z[here, LANES:]), (filt_ref[0], filt_ref[1]))
        sections.append(jnp.concatenate(turned, axis=1))
    z = dot_table(jnp.concatenate(sections, axis=0), backward_ref, PASSES[2])
    sections = []
    for q in range(pulses):
        here = slice(q * radix, (q + 1) * radix)
        turned = complex_times((z[here, :LANES], z[here, LANES:]), (twiddle_ref[0], twiddle_ref[1]))
        sections.append(jnp.concatenate(turned, axis=0))
    y = table_dot(last_ref, jnp.concatenate(sections, axis=1), PASSES[3])
    for q in range(pulses):
        shift = shifts_ref[me * pulses + q]
        source = lane + shift
        for part in range(2):
            cells = y[part * radix : (part + 1) * radix, q * LANES : (q + 1) * LANES]
            turned = pltpu.roll(cells, lax.rem(LANES - shift, LANES), 1)
            after = jnp.where(row == radix - 1, 0.0, pltpu.roll(turned, radix - 1, 0))
            before = jnp.where(row == 0, 0.0, pltpu.roll(turned, 1, 0))
            moved = jnp.where(source >= LANES, after, jnp.where(source < 0, before, turned))
            total[pl.ds(part * pulses + q, radix, stride=wide), :] = moved

    length = radix // ranks * wide
    for d in range(ranks):
        start = pl.multiple_of(lax.bitwise_xor(me, d) * length, 8)
        target = odd if d % 2 else near
        target[d // 2] = total[pl.ds(start, length), :].astype(BF16)


def compress(echoes, filter_spectrum, range_shifts, steering, tap_offsets, tap_weights, phase_rates, me, ranks):
    pulses, _, samples = echoes.shape
    radix = samples // LANES
    wide = 2 * pulses
    view = echoes.reshape(pulses, 2, radix, LANES).transpose(0, 2, 1, 3)
    view = view.reshape(pulses, 2 * radix, LANES)
    filt = filter_spectrum.reshape(2, radix, LANES).transpose(1, 0, 2).reshape(2 * radix, LANES)
    angles = steering.shape[2]
    steer = steering.reshape(2 * angles, -1)
    first, forward, backward, last, twiddle = [jnp.asarray(t) for t in dft_tables(samples)]
    loads = [view, first, twiddle, filt, forward, backward, last]
    loads += [tap_weights, tap_offsets, phase_rates, steer]
    smem = pl.BlockSpec(memory_space=pltpu.SMEM)
    vmem = pl.BlockSpec(memory_space=pltpu.VMEM)
    away = pl.BlockSpec(memory_space=pltpu.HBM)
    half = ranks // 2
    return pl.pallas_call(
        functools.partial(compress_kernel, ranks),
        out_shape=[
            jax.ShapeDtypeStruct((half, radix // ranks * wide, LANES), BF16) for _ in range(2)
        ]
        + [jax.ShapeDtypeStruct((2 * angles + 48 * angles // LANES, steer.shape[1]), BF16)],
        in_specs=[smem, smem] + [away] * LOADS,
        out_specs=[vmem] * 3,
        scratch_shapes=[pltpu.VMEM((radix * wide, LANES), F32), pltpu.VMEM((2, radix, LANES), F32)]
        + [pltpu.VMEM(x.shape, x.dtype) for x in loads[:-1]]
        + [pltpu.SemaphoreType.DMA((LOADS + pulses // QUAD,))],
        compiler_params=pltpu.CompilerParams(vmem_limit_bytes=COMPRESS_LIMIT),
        cost_estimate=pl.CostEstimate(
            flops=pulses * samples * 4000, bytes_accessed=pulses * samples * 12, transcendentals=0
        ),
        name="compress",
    )(me, range_shifts, *loads)


def pack_kernel(cuts, wide, *refs):
    near, far, *outs = refs
    half = far.shape[0]
    for cut, (low, high) in enumerate(cuts):
        for z in range(half):
            outs[cut * half + z][0] = near[z, low * wide : high * wide]
            outs[cut * half + z][1] = far[z, low * wide : high * wide]


def pack(near, far, cuts, wide):
    half = far.shape[0]
    vmem = pl.BlockSpec(memory_space=pltpu.VMEM)
    flat = pl.pallas_call(
        functools.partial(pack_kernel, cuts, wide),
        out_shape=[
            jax.ShapeDtypeStruct((2, (high - low) * wide, LANES), BF16)
            for low, high in cuts
            for _ in range(half)
        ],
        in_specs=[vmem] * 2,
        out_specs=[vmem] * (len(cuts) * half),
        compiler_params=pltpu.CompilerParams(vmem_limit_bytes=16 * 1024 * 1024),
        cost_estimate=pl.CostEstimate(flops=1 << 20, bytes_accessed=1 << 20, transcendentals=0),
        name="pack",
    )(near, far)
    return [flat[cut * half : (cut + 1) * half] for cut in range(len(cuts))]


def twice(a):
    double = a[1] + a[1]
    return 1.0 - double * a[1], double * a[0]


def complex_times(a, b):
    return a[0] * b[0] - a[1] * b[1], a[0] * b[1] + a[1] * b[0]


def prepare_kernel(groups, ranks, rows, samples, pair, cuts, me_ref, *refs):
    steer = refs[:groups]
    mixes, mats, *turns = refs[groups:]
    places = [(cut, at) for cut, (low, high) in enumerate(cuts) for at in range((high - low) // pair)]
    angles = mats.shape[-1]
    members = steer[0].shape[-1]
    me = me_ref[0]
    share = members // ranks
    column = lax.broadcasted_iota(jnp.int32, (members, 2 * members), 1)
    member = lax.broadcasted_iota(jnp.int32, (members, 2 * members), 0)
    slot = lax.div(column, 2 * share)
    within = lax.rem(column, 2 * share)
    part = lax.div(within, share)
    source = lax.bitwise_xor(slot, me) * share + lax.rem(within, share)
    picks = [
        jnp.where((part == c) & (source == member), 1.0, 0.0).astype(BF16) for c in range(2)
    ]
    below = lax.broadcasted_iota(jnp.int32, (angles, angles), 0)
    across = lax.broadcasted_iota(jnp.int32, (1, angles), 1)
    lane = lax.broadcasted_iota(jnp.int32, (angles, LANES), 1)
    small = lane.astype(F32) * (1.0 / samples)
    tables = [decode(steer[2 * pick], 2 * angles, angles) for pick in range(groups // 2)]
    rates = jnp.concatenate([table[10:12] for table in tables], axis=0)
    begin = rates * ((me * (rows * LANES)).astype(F32) * (1.0 / samples))
    lines = [rates, jnp.cos(begin), jnp.sin(begin)]
    for count in (1, pair):
        phase = rates * (count * LANES / samples)
        lines += [jnp.cos(phase), jnp.sin(phase)]
    lines.append(jnp.zeros((LANES - 7 * groups, angles), F32))
    lines = jnp.transpose(jnp.concatenate(lines, axis=0))

    def spread(kind, n):
        at = kind * groups + n
        return jnp.broadcast_to(lines[:, at : at + 1], (angles, LANES))

    for pick in range(groups // 2):
        offset = 2 * pick
        table = tables[pick]
        for h in range(2):
            moved = table[8 + h : 9 + h, :].astype(jnp.int32)
            total = jnp.zeros((angles, angles), F32)
            for tap in range(4):
                at_row = jnp.clip(across + moved + (tap - 1), 0, angles - 1)
                total = total + jnp.where(below == at_row, table[4 * h + tap : 4 * h + tap + 1, :], 0.0)
            matrix = jnp.transpose(total).astype(BF16)
            mats[2 * pick + h] = matrix
            near = steer[offset ^ h]
            real = dot(matrix, near[:angles, :]).astype(BF16)
            imag = dot(matrix, near[angles : 2 * angles, :]).astype(BF16)
            mixes[2 * pick + h, :angles, :] = (dot(real, picks[0]) - dot(imag, picks[1])).astype(BF16)
            mixes[2 * pick + h, angles:, :] = (dot(imag, picks[0]) + dot(real, picks[1])).astype(BF16)
            n = 2 * pick + h
            now = complex_times((spread(1, n), spread(2, n)), small_turn(spread(0, n) * small))
            first = now
            step = (spread(3, n), spread(4, n))
            for u in range(pair):
                here = slice(u * LANES, (u + 1) * LANES)
                if u:
                    first = complex_times(first, step)
                now = first
                jump = (spread(5, n), spread(6, n))
                for index, (cut, at) in enumerate(places):
                    if index:
                        now = complex_times(now, jump)
                    turns[cut][at, n, 0, :, here], turns[cut][at, n, 1, :, here] = now


def small_turn(x):
    y = x * x
    cosine = 1.0 - y * (0.5 - y * (1.0 / 24.0 - y * (1.0 / 720.0)))
    return cosine, x * (1.0 - y * (1.0 / 6.0 - y * (1.0 / 120.0 - y * (1.0 / 5040.0))))


def prepare(steer, angles, me, groups, ranks, rows, samples, pair, cuts):
    members = steer[0].shape[1]
    smem = pl.BlockSpec(memory_space=pltpu.SMEM)
    vmem = pl.BlockSpec(memory_space=pltpu.VMEM)
    return pl.pallas_call(
        functools.partial(prepare_kernel, groups, ranks, rows, samples, pair, cuts),
        out_shape=[
            jax.ShapeDtypeStruct((groups, 2 * angles, 2 * members), BF16),
            jax.ShapeDtypeStruct((groups, angles, angles), BF16),
        ]
        + [
            jax.ShapeDtypeStruct(((high - low) // pair, groups, 2, angles, pair * LANES), F32)
            for low, high in cuts
        ],
        in_specs=[smem] + [vmem] * len(steer),
        out_specs=[vmem] * (2 + len(cuts)),
        compiler_params=pltpu.CompilerParams(vmem_limit_bytes=32 * 1024 * 1024),
        cost_estimate=pl.CostEstimate(
            flops=groups * angles * members * 40000, bytes_accessed=8 << 20, transcendentals=0
        ),
        name="prepare",
    )(me, *steer)


BAND = 32


def direct(source):
    return source & (source - 1) == 0


def kinds(groups):
    whole = [p for p in range(groups // 2) if direct(2 * p) and direct(2 * p + 1)]
    half = [p for p in range(groups // 2) if direct(2 * p) and not direct(2 * p + 1)]
    return whole, half


def columns(parts, wide, base, pair):
    return jnp.concatenate(
        [
            jnp.concatenate(
                [
                    ref[:, pl.ds(pl.multiple_of((base + u) * wide, 8), wide), :].reshape(-1, LANES)
                    for ref in parts
                ],
                axis=0,
            )
            for u in range(pair)
        ],
        axis=1,
    )


def rotated(mixed, turns, at, n, level, top, angles):
    band = slice(top, top + BAND)
    lower = slice(angles + top, angles + top + BAND)
    now = (turns[at, n, 0, band], turns[at, n, 1, band])
    power = twice(now) if level else now
    for _ in range(level - 1):
        power = complex_times(power, now)
    return complex_times((mixed[n, band], mixed[n, lower]), power)


def add(a, b):
    return a[0] + b[0], a[1] + b[1]


def near_kernel(groups, count, layout, mixes, turns, *refs):
    image, partial, mixed = refs[-3:]
    held = split(refs[:-3], layout)
    whole, half = kinds(groups)
    pair, angles = turns.shape[-1] // LANES, turns.shape[-2]
    wide = held[0][0].shape[1] // (count * pair)

    @pl.loop(0, count)
    def _(step):
        here = step
        cells = {o: columns(parts, wide, step * pair, pair) for o, parts in held.items()}
        ready = [n for n in range(groups) if direct(n)]
        for n in ready:
            mixed[n] = dot(mixes[n], cells[n])
        for pick in range(groups // 2):
            terms = [n for n in (2 * pick, 2 * pick + 1) if n in ready]
            for top in range(0, angles if terms else 0, BAND):
                band = slice(top, top + BAND)
                total = rotated(mixed, turns, here, terms[0], 0, top, angles)
                if len(terms) == 2:
                    total = add(total, rotated(mixed, turns, here, terms[1], 0, top, angles))
                    side = pair * LANES
                    image[step, whole.index(pick), band, :side] = total[0].astype(BF16)
                    image[step, whole.index(pick), band, side:] = total[1].astype(BF16)
                else:
                    spot = half.index(pick)
                    partial[step, spot, 0, band], partial[step, spot, 1, band] = total


def far_kernel(groups, count, layout, unit, mixes, mats, turns, image, partial, *refs):
    out, mixed, images = refs[-3:]
    held = split(refs[: sum(len(parts) for parts in layout.values())], layout)
    levels = groups.bit_length() - 1
    whole, half = kinds(groups)
    pair, angles = turns.shape[-1] // LANES, turns.shape[-2]
    wide = held[groups - 1][0].shape[1] // (count * pair)
    side = pair * LANES
    started = pl.program_id(0) * (unit // pair)
    middle = angles // 2
    window = min(angles, -(-(middle + REACH) // LANES) * LANES)
    if len(out.shape) == 3:
        out = out.reshape(out.shape[0] * out.shape[1], LANES)

    @pl.loop(0, unit // pair)
    def _(step):
        place = started + step
        here = place
        cells = {o: columns(parts, wide, place * pair, pair) for o, parts in held.items()}
        late = [n for n in range(groups) if n in held]
        for n in late:
            mixed[n] = dot(mixes[n], cells[n])
        for pick in range(groups // 2):
            terms = [n for n in (2 * pick, 2 * pick + 1) if n in late]
            if not terms:
                images[pick] = image[place, whole.index(pick)]
                continue
            for top in range(0, angles, BAND):
                band = slice(top, top + BAND)
                total = rotated(mixed, turns, here, terms[0], 0, top, angles)
                if len(terms) == 2:
                    total = add(total, rotated(mixed, turns, here, terms[1], 0, top, angles))
                else:
                    spot = half.index(pick)
                    total = add(total, (partial[place, spot, 0, band], partial[place, spot, 1, band]))
                images[pick, band, :side] = total[0].astype(BF16)
                images[pick, band, side:] = total[1].astype(BF16)
        for level in range(1, levels):
            last = level == levels - 1
            stride = 2 << level
            for offset in range(0, groups, stride):
                for h in range(2):
                    n = offset + h
                    source = images.at[(offset ^ (h << level)) // 2]
                    for low, high, start in ((0, middle, 0), (middle, angles, angles - window)):
                        turned = dot(mats[n, low:high, start : start + window], source[start : start + window])
                        mixed[n, low:high] = turned[:, :side]
                        mixed[n, angles + low : angles + high] = turned[:, side:]
            for offset in range(0, groups, stride):
                for top in range(0, angles, BAND):
                    band = slice(top, top + BAND)
                    re, im = add(
                        rotated(mixed, turns, here, offset, level, top, angles),
                        rotated(mixed, turns, here, offset + 1, level, top, angles),
                    )
                    if not last:
                        images[offset // 2, band, :side] = re.astype(BF16)
                        images[offset // 2, band, side:] = im.astype(BF16)
                        continue
                    for u in range(pair):
                        lanes = slice(u * LANES, (u + 1) * LANES)
                        spot = top * unit * 2 + (step * pair + u) * 2
                        out[pl.ds(spot, BAND, stride=unit * 2), :] = re[:, lanes]
                        out[pl.ds(spot + 1, BAND, stride=unit * 2), :] = im[:, lanes]


def split(refs, layout):
    held, at = {}, 0
    for offset, parts in layout.items():
        held[offset] = refs[at : at + len(parts)]
        at += len(parts)
    return held


def merge_near(held, mixes, turns, low, high):
    groups, pair, angles = mixes.shape[0], turns.shape[-1] // LANES, turns.shape[-2]
    vmem = pl.BlockSpec(memory_space=pltpu.VMEM)
    count = (high - low) // pair
    whole, half = kinds(groups)
    flat = [part for parts in held.values() for part in parts]
    return pl.pallas_call(
        functools.partial(near_kernel, groups, count, held),
        out_shape=[
            jax.ShapeDtypeStruct((count, len(whole), angles, 2 * pair * LANES), BF16),
            jax.ShapeDtypeStruct((count, len(half), 2, angles, pair * LANES), F32),
        ],
        in_specs=[vmem] * (2 + len(flat)),
        out_specs=[vmem] * 2,
        scratch_shapes=[pltpu.VMEM((groups, 2 * angles, pair * LANES), F32)],
        compiler_params=pltpu.CompilerParams(vmem_limit_bytes=MERGE_LIMIT),
        cost_estimate=pl.CostEstimate(
            flops=groups * angles * angles * (high - low) * LANES * 4,
            bytes_accessed=angles * (high - low) * LANES * 8,
            transcendentals=0,
        ),
        name="merge_near",
    )(mixes, turns, *flat)


def merge_far(held, mixes, mats, turns, image, partial, rows, low, high, unit, before):
    groups, pair, angles = mixes.shape[0], turns.shape[-1] // LANES, turns.shape[-2]
    vmem = pl.BlockSpec(memory_space=pltpu.VMEM)
    flat = [part for parts in held.values() for part in parts]
    if unit * 2 % 8:
        shape, block, spot = (angles * rows * 2, LANES), (angles * unit * 2, LANES), lambda i: (0, 0)
    else:
        shape, block = (angles, rows * 2, LANES), (angles, unit * 2, LANES)
        spot = lambda i: (0, low // unit + i, 0)
    operands = [mixes, mats, turns, image, partial, *flat]
    specs = [vmem] * len(operands)
    aliases = {}
    if before is not None:
        aliases[len(operands)] = 0
        operands.append(before)
        specs.append(pl.BlockSpec(memory_space=pltpu.HBM))
    return pl.pallas_call(
        functools.partial(far_kernel, groups, (high - low) // pair, held, unit),
        grid=((high - low) // unit,),
        out_shape=jax.ShapeDtypeStruct(shape, F32),
        in_specs=specs,
        out_specs=pl.BlockSpec(block, spot),
        input_output_aliases=aliases,
        scratch_shapes=[
            pltpu.VMEM((groups, 2 * angles, pair * LANES), F32),
            pltpu.VMEM((groups // 2, angles, 2 * pair * LANES), BF16),
        ],
        compiler_params=pltpu.CompilerParams(vmem_limit_bytes=MERGE_LIMIT),
        cost_estimate=pl.CostEstimate(
            flops=groups * angles * angles * (high - low) * LANES * 4,
            bytes_accessed=angles * (high - low) * LANES * 16,
            transcendentals=0,
        ),
        name="merge_far",
    )(*operands)


def hop(value, axis, offset):
    if not offset:
        return value
    return lax.ppermute(value, axis, [(i, i ^ offset) for i in range(lax.axis_size(axis))])


def neighbours(x, groups):
    return {1 << b: hop(x, "sub", 1 << b) for b in range(groups.bit_length() - 1)}


def others(x, near, groups):
    held = {0: [x]}
    for bit in near:
        held[bit] = [near[bit]]
    slots = x.shape[0]
    for offset in range(groups):
        if offset in held:
            continue
        via = [bit for bit in near if offset & bit]
        edges = [slots * i // len(via) for i in range(len(via) + 1)]
        pieces = []
        for bit, low, high in zip(via, edges[:-1], edges[1:]):
            source = held[offset ^ bit]
            source = source[0] if len(source) == 1 else jnp.concatenate(source, axis=0)
            pieces.append(hop(source[low:high], "sub", bit))
        held[offset] = pieces
    return [held[offset] for offset in range(groups)]


def local(echoes, filter_spectrum, range_shifts, steering, tap_offsets, tap_weights, phase_rates):
    ranks, groups = lax.axis_size("rng"), lax.axis_size("sub")
    pulses, _, samples = echoes.shape
    rows = samples // LANES // ranks
    angles = steering.shape[2]
    me = lax.axis_index("rng").astype(jnp.int32).reshape(1)
    unit = UNIT if rows % UNIT == 0 else rows
    cuts = [(low, low + unit) for low in range(0, rows, unit)]
    batches = [(0, unit)] + ([(unit, rows)] if unit < rows else [])

    near, odd, early = compress(
        echoes, filter_spectrum, range_shifts, steering, tap_offsets, tap_weights, phase_rates,
        me, ranks,
    )
    steers = [hop(early, "sub", e) for e in range(groups)]
    wide = 2 * pulses
    packed = pack(near, hop(odd, "rng", 1), batches, wide)
    batch = []
    for blocks in packed:
        batch.append([hop(block, "rng", 2 * z) for z, block in enumerate(blocks)])
    arrived = [jnp.concatenate(batch[0], axis=0)]
    steers, _ = lax.optimization_barrier((steers, arrived[0]))
    pair = 2 if unit % 2 == 0 else 1
    ready = prepare(steers, angles, me, groups, ranks, rows, samples, pair, cuts)
    if len(batch) > 1:
        batch[1], ready = lax.optimization_barrier((batch[1], ready))
        for at in range(0, batch[1][0].shape[1], unit * wide):
            pieces = [piece[:, at : at + unit * wide] for piece in batch[1]]
            arrived.append(jnp.concatenate(pieces, axis=0))
    mixes, mats, *turns = ready

    nears = []
    for x in arrived:
        nears.append(neighbours(x, groups))
    out = None
    for cut, (low, high) in enumerate(cuts):
        held = others(arrived[cut], nears[cut], groups)
        close = {o: held[o] for o in range(groups) if direct(o)}
        far = {o: held[o] for o in range(groups) if not direct(o)}
        image, partial = merge_near(close, mixes, turns[cut], low, high)
        if cut and cut + 1 < len(cuts):
            nears[cut + 1], image = lax.optimization_barrier((nears[cut + 1], image))
        out = merge_far(far, mixes, mats, turns[cut], image, partial, rows, low, high, unit, out)
        if not cut and len(cuts) > 1:
            nears[1], out = lax.optimization_barrier((nears[1], out))
    out = out.reshape(angles, rows, 2, LANES).transpose(0, 2, 1, 3)
    out = with_layout_constraint(out, Layout(major_to_minor=(0, 2, 1, 3)))
    return out.reshape(angles, 2, rows * LANES)


def solution(mesh):
    placed = (
        P(("sub", "rng"), None, None),
        P(),
        P("sub"),
        P("sub", None, None, None),
        P("sub", None, None),
        P("sub", None, None, None),
        P("sub", None, None),
    )

    return jax.shard_map(
        local, mesh=mesh, in_specs=placed, out_specs=P("sub", None, "rng"), check_vma=False
    )
```

```python
import functools
import math

import jax
import jax.numpy as jnp
import numpy as np
from jax import lax
from jax.experimental import pallas as pl
from jax.experimental.layout import Layout, with_layout_constraint
from jax.experimental.pallas import tpu as pltpu
from jax.sharding import PartitionSpec as P


LANES = 128
QUAD = 4
F32 = jnp.float32
BF16 = jnp.bfloat16
MERGE_LIMIT = 16 * 1024 * 1024
REACH = 6
UNIT = 4
LOADS = 11
PASSES = (3, 3, 1, 1)
COMPRESS_LIMIT = 60 * 1024 * 1024


def split_table(table):
    high = table.astype(np.float32).astype(BF16)
    low = (table - high.astype(np.float64)).astype(np.float32).astype(BF16)
    return np.stack([high, low])


def frequency_order(radix):
    sections = math.lcm(radix, LANES) // radix
    place = np.arange(LANES)
    return sections * (place % (LANES // sections)) + place // (LANES // sections)


@functools.lru_cache(None)
def dft_tables(samples):
    radix = samples // LANES
    outer = 2.0 * np.pi * (np.outer(np.arange(radix), np.arange(radix)) % radix) / radix
    inner = 2.0 * np.pi * (np.outer(np.arange(LANES), np.arange(LANES)) % LANES) / LANES
    turn = 2.0 * np.pi * np.outer(np.arange(radix), np.arange(LANES)) / samples
    c, s = np.cos(outer), np.sin(outer)
    first = np.concatenate(
        [np.stack([c, s], -1).reshape(radix, -1), np.stack([-s, c], -1).reshape(radix, -1)]
    )
    last = np.block([[c, -s], [s, c]]) / samples
    order = frequency_order(radix)
    c, s = np.cos(inner)[:, order], np.sin(inner)[:, order]
    forward = np.block([[c, -s], [s, c]])
    backward = np.block([[c.T, s.T], [-s.T, c.T]])
    twiddle = np.stack([np.cos(turn), np.sin(turn)]).astype(np.float32)
    return (
        split_table(first),
        split_table(forward),
        split_table(backward),
        split_table(last),
        twiddle,
    )


def halves(x):
    high = x.astype(BF16)
    return high, (x - high.astype(F32)).astype(BF16)


def dot(a, b):
    return jnp.dot(a, b, preferred_element_type=F32)


def table_dot(table, x, passes=3):
    if passes == 1:
        return dot(table[0], x.astype(BF16))
    high, low = halves(x)
    if passes == 2:
        return dot(table[0], high) + dot(table[0], low)
    return dot(table[0], high) + dot(table[0], low) + dot(table[1], high)


def dot_table(x, table, passes=3):
    if passes == 1:
        return dot(x.astype(BF16), table[0])
    high, low = halves(x)
    if passes == 2:
        return dot(high, table[0]) + dot(low, table[0])
    return dot(high, table[0]) + dot(low, table[0]) + dot(high, table[1])


def encode(early, base, taps_ref, offsets_ref, rates_ref):
    angles = rates_ref.shape[-1]
    empty = jnp.zeros((4, angles), F32)
    left = jnp.concatenate(
        [taps_ref[0, 0], taps_ref[0, 1], offsets_ref[0].astype(F32), rates_ref[0], empty], axis=0
    )
    for piece in range(3):
        high = left.astype(BF16)
        left = left - high.astype(F32)
        for at in range(angles // LANES):
            spot = base + 16 * (piece * (angles // LANES) + at)
            early[spot : spot + 16, :LANES] = high[:, at * LANES : (at + 1) * LANES]


def decode(ref, base, angles):
    pieces = []
    for piece in range(3):
        spots = [base + 16 * (piece * (angles // LANES) + at) for at in range(angles // LANES)]
        pieces.append(
            jnp.concatenate([ref[spot : spot + 16, :LANES] for spot in spots], axis=1).astype(F32)
        )
    return pieces[0] + pieces[1] + pieces[2]


def load_filter(raw_ref, filt_ref):
    radix = filt_ref.shape[1]
    period = math.lcm(radix, LANES)
    sections, rows = period // radix, period // LANES
    count = LANES // sections
    lane = lax.broadcasted_iota(jnp.int32, (count, LANES), 1)
    for part in range(2):
        near = [raw_ref[pl.ds(2 * o + part, count, stride=2 * rows), :] for o in range(rows)]
        stack = []
        for u in range(sections):
            at, skip = divmod(radix * u, LANES)
            cells = near[at]
            if skip:
                cells = pltpu.roll(cells, LANES - skip, 1)
                if skip + radix > LANES:
                    after = pltpu.roll(near[at + 1], LANES - skip, 1)
                    cells = jnp.where(lane < LANES - skip, cells, after)
            stack.append(cells)
        filt_ref[part] = jnp.transpose(jnp.concatenate(stack, axis=0))[:radix]


def compress_kernel(ranks, me_ref, shifts_ref, *refs):
    loads, (near_out, odd_out, early_out) = refs[:LOADS], refs[LOADS : LOADS + 3]
    total, filt_ref, near, odd, early, *held = refs[LOADS + 3 : -2]
    done, sent = refs[-2:]
    echo_ref, first_ref, twiddle_ref, raw_ref, forward_ref, backward_ref, last_ref = held[:7]
    taps_ref, offsets_ref, rates_ref = held[7:]
    held = [*held, early.at[pl.ds(0, loads[-1].shape[0])]]

    def piece(step):
        cells = pl.ds(step * QUAD, QUAD)
        return pltpu.make_async_copy(
            loads[0].at[cells], echo_ref.at[cells], done.at[LOADS + step]
        )

    copies = [pltpu.make_async_copy(loads[i], held[i], done.at[i]) for i in range(1, LOADS)]
    first, twiddle, raw, forward, backward, last = copies[:6]
    first.start()
    piece(0).start()
    twiddle.start()
    for step in range(1, echo_ref.shape[0] // QUAD):
        piece(step).start()
    for copy in (*copies[6:], raw, forward, backward, last):
        copy.start()
    first.wait()
    pulses, radix = echo_ref.shape[0], echo_ref.shape[1] // 2
    wide = 2 * pulses
    me = me_ref[0]
    lane = lax.broadcasted_iota(jnp.int32, (radix, LANES), 1)
    row = lax.broadcasted_iota(jnp.int32, (radix, LANES), 0)
    sections = []
    for step in range(pulses // QUAD):
        piece(step).wait()
        x = jnp.concatenate([echo_ref[step * QUAD + q] for q in range(QUAD)], axis=1)
        y = table_dot(first_ref, x, PASSES[0])
        if not step:
            twiddle.wait()
        for q in range(QUAD):
            here = slice(q * LANES, (q + 1) * LANES)
            turned = complex_times((y[:radix, here], y[radix:, here]), (twiddle_ref[0], -twiddle_ref[1]))
            sections.append(jnp.concatenate(turned, axis=1))
    for copy in (*copies[6:], raw, forward, backward, last):
        copy.wait()
    load_filter(raw_ref, filt_ref)
    encode(early, loads[-1].shape[0], taps_ref, offsets_ref, rates_ref)
    sends = [pltpu.make_async_copy(early, early_out, sent.at[ranks])]
    sends[0].start()
    z = dot_table(jnp.concatenate(sections, axis=0), forward_ref, PASSES[1])
    sections = []
    for q in range(pulses):
        here = slice(q * radix, (q + 1) * radix)
        turned = complex_times((z[here, :LANES], z[here, LANES:]), (filt_ref[0], filt_ref[1]))
        sections.append(jnp.concatenate(turned, axis=1))
    z = dot_table(jnp.concatenate(sections, axis=0), backward_ref, PASSES[2])
    sections = []
    for q in range(pulses):
        here = slice(q * radix, (q + 1) * radix)
        turned = complex_times((z[here, :LANES], z[here, LANES:]), (twiddle_ref[0], twiddle_ref[1]))
        sections.append(jnp.concatenate(turned, axis=0))
    y = table_dot(last_ref, jnp.concatenate(sections, axis=1), PASSES[3])
    for q in range(pulses):
        shift = shifts_ref[me * pulses + q]
        source = lane + shift
        for part in range(2):
            cells = y[part * radix : (part + 1) * radix, q * LANES : (q + 1) * LANES]
            turned = pltpu.roll(cells, lax.rem(LANES - shift, LANES), 1)
            after = jnp.where(row == radix - 1, 0.0, pltpu.roll(turned, radix - 1, 0))
            before = jnp.where(row == 0, 0.0, pltpu.roll(turned, 1, 0))
            moved = jnp.where(source >= LANES, after, jnp.where(source < 0, before, turned))
            total[pl.ds(part * pulses + q, radix, stride=wide), :] = moved

    length = radix // ranks * wide
    for d in (*range(1, ranks, 2), *range(0, ranks, 2)):
        start = pl.multiple_of(lax.bitwise_xor(me, d) * length, 8)
        staged, target = (odd, odd_out) if d % 2 else (near, near_out)
        staged[d // 2] = total[pl.ds(start, length), :].astype(BF16)
        sends.append(pltpu.make_async_copy(staged.at[d // 2], target.at[d // 2], sent.at[d]))
        sends[-1].start()
    for copy in sends:
        copy.wait()


def compress(echoes, filter_spectrum, range_shifts, steering, tap_offsets, tap_weights, phase_rates, me, ranks):
    pulses, _, samples = echoes.shape
    radix = samples // LANES
    wide = 2 * pulses
    view = echoes.reshape(pulses, 2, radix, LANES).transpose(0, 2, 1, 3)
    view = view.reshape(pulses, 2 * radix, LANES)
    filt = filter_spectrum.reshape(2, radix, LANES).transpose(1, 0, 2).reshape(2 * radix, LANES)
    angles = steering.shape[2]
    steer = steering.reshape(2 * angles, -1)
    first, forward, backward, last, twiddle = [jnp.asarray(t) for t in dft_tables(samples)]
    loads = [view, first, twiddle, filt, forward, backward, last]
    loads += [tap_weights, tap_offsets, phase_rates, steer]
    smem = pl.BlockSpec(memory_space=pltpu.SMEM)
    vmem = pl.BlockSpec(memory_space=pltpu.VMEM)
    away = pl.BlockSpec(memory_space=pltpu.HBM)
    half = ranks // 2
    return pl.pallas_call(
        functools.partial(compress_kernel, ranks),
        out_shape=[
            jax.ShapeDtypeStruct((half, radix // ranks * wide, LANES), BF16) for _ in range(2)
        ]
        + [jax.ShapeDtypeStruct((2 * angles + 48 * angles // LANES, steer.shape[1]), BF16)],
        in_specs=[smem, smem] + [away] * LOADS,
        out_specs=[away] * 3,
        scratch_shapes=[pltpu.VMEM((radix * wide, LANES), F32), pltpu.VMEM((2, radix, LANES), F32)]
        + [pltpu.VMEM((half, radix // ranks * wide, LANES), BF16) for _ in range(2)]
        + [pltpu.VMEM((2 * angles + 48 * angles // LANES, steer.shape[1]), BF16)]
        + [pltpu.VMEM(x.shape, x.dtype) for x in loads[:-1]]
        + [pltpu.SemaphoreType.DMA((LOADS + pulses // QUAD,)), pltpu.SemaphoreType.DMA((ranks + 1,))],
        compiler_params=pltpu.CompilerParams(vmem_limit_bytes=COMPRESS_LIMIT),
        cost_estimate=pl.CostEstimate(
            flops=pulses * samples * 4000, bytes_accessed=pulses * samples * 12, transcendentals=0
        ),
        name="compress",
    )(me, range_shifts, *loads)


def pack_kernel(cuts, wide, *refs):
    near, far, *outs = refs
    half = far.shape[0]
    for cut, (low, high) in enumerate(cuts):
        for z in range(half):
            outs[cut * half + z][0] = near[z, low * wide : high * wide]
            outs[cut * half + z][1] = far[z, low * wide : high * wide]


def pack(near, far, cuts, wide):
    half = far.shape[0]
    vmem = pl.BlockSpec(memory_space=pltpu.VMEM)
    flat = pl.pallas_call(
        functools.partial(pack_kernel, cuts, wide),
        out_shape=[
            jax.ShapeDtypeStruct((2, (high - low) * wide, LANES), BF16)
            for low, high in cuts
            for _ in range(half)
        ],
        in_specs=[vmem] * 2,
        out_specs=[vmem] * (len(cuts) * half),
        compiler_params=pltpu.CompilerParams(vmem_limit_bytes=16 * 1024 * 1024),
        cost_estimate=pl.CostEstimate(flops=1 << 20, bytes_accessed=1 << 20, transcendentals=0),
        name="pack",
    )(near, far)
    return [flat[cut * half : (cut + 1) * half] for cut in range(len(cuts))]


def twice(a):
    double = a[1] + a[1]
    return 1.0 - double * a[1], double * a[0]


def complex_times(a, b):
    return a[0] * b[0] - a[1] * b[1], a[0] * b[1] + a[1] * b[0]


def prepare_kernel(groups, ranks, rows, samples, pair, me_ref, *refs):
    steer = refs[:groups]
    mixes, mats, strides, turns = refs[groups:]
    angles = mats.shape[-1]
    members = steer[0].shape[-1]
    me = me_ref[0]
    share = members // ranks
    column = lax.broadcasted_iota(jnp.int32, (members, 2 * members), 1)
    member = lax.broadcasted_iota(jnp.int32, (members, 2 * members), 0)
    slot = lax.div(column, 2 * share)
    within = lax.rem(column, 2 * share)
    part = lax.div(within, share)
    source = lax.bitwise_xor(slot, me) * share + lax.rem(within, share)
    picks = [
        jnp.where((part == c) & (source == member), 1.0, 0.0).astype(BF16) for c in range(2)
    ]
    below = lax.broadcasted_iota(jnp.int32, (angles, angles), 0)
    across = lax.broadcasted_iota(jnp.int32, (1, angles), 1)
    lane = lax.broadcasted_iota(jnp.int32, (angles, LANES), 1)
    small = lane.astype(F32) * (1.0 / samples)
    tables = [decode(steer[2 * pick], 2 * angles, angles) for pick in range(groups // 2)]
    rates = jnp.concatenate([table[10:12] for table in tables], axis=0)
    begin = rates * ((me * (rows * LANES)).astype(F32) * (1.0 / samples))
    lines = [rates, jnp.cos(begin), jnp.sin(begin)]
    for count in (1, pair):
        phase = rates * (count * LANES / samples)
        lines += [jnp.cos(phase), jnp.sin(phase)]
    lines.append(jnp.zeros((LANES - 7 * groups, angles), F32))
    lines = jnp.transpose(jnp.concatenate(lines, axis=0))

    def spread(kind, n):
        at = kind * groups + n
        return jnp.broadcast_to(lines[:, at : at + 1], (angles, LANES))

    for pick in range(groups // 2):
        offset = 2 * pick
        table = tables[pick]
        for h in range(2):
            moved = table[8 + h : 9 + h, :].astype(jnp.int32)
            total = jnp.zeros((angles, angles), F32)
            for tap in range(4):
                at_row = jnp.clip(across + moved + (tap - 1), 0, angles - 1)
                total = total + jnp.where(below == at_row, table[4 * h + tap : 4 * h + tap + 1, :], 0.0)
            matrix = jnp.transpose(total).astype(BF16)
            mats[2 * pick + h] = matrix
            near = steer[offset ^ h]
            real = dot(matrix, near[:angles, :]).astype(BF16)
            imag = dot(matrix, near[angles : 2 * angles, :]).astype(BF16)
            mixes[2 * pick + h, :angles, :] = (dot(real, picks[0]) - dot(imag, picks[1])).astype(BF16)
            mixes[2 * pick + h, angles:, :] = (dot(imag, picks[0]) + dot(real, picks[1])).astype(BF16)
            n = 2 * pick + h
            now = complex_times((spread(1, n), spread(2, n)), small_turn(spread(0, n) * small))
            first = now
            step = (spread(3, n), spread(4, n))
            for u in range(pair):
                here = slice(u * LANES, (u + 1) * LANES)
                if u:
                    first = complex_times(first, step)
                now = first
                jump = (spread(5, n), spread(6, n))
                for at in range(turns.shape[0]):
                    if at:
                        now = complex_times(now, jump)
                    turns[at, n, 0, :, here], turns[at, n, 1, :, here] = now
            strides[n, 0], strides[n, 1] = jump


def spin_kernel(strides, start, *turns):
    last, groups, _, angles, side = start.shape
    for n in range(groups):
        for top in range(0, angles, BAND):
            band = slice(top, top + BAND)
            jump = (strides[n, 0, band], strides[n, 1, band])
            for at in range(0, side, LANES):
                here = slice(at, at + LANES)
                now = (start[last - 1, n, 0, band, here], start[last - 1, n, 1, band, here])
                for turn in turns:
                    for place in range(last):
                        now = complex_times(now, jump)
                        turn[place, n, 0, band, here], turn[place, n, 1, band, here] = now


def spin(strides, start, count):
    vmem = pl.BlockSpec(memory_space=pltpu.VMEM)
    return pl.pallas_call(
        spin_kernel,
        out_shape=[jax.ShapeDtypeStruct(start.shape, F32)] * count,
        in_specs=[vmem] * 2,
        out_specs=[vmem] * count,
        compiler_params=pltpu.CompilerParams(vmem_limit_bytes=MERGE_LIMIT),
        cost_estimate=pl.CostEstimate(
            flops=6 * count * start.size, bytes_accessed=4 * start.size, transcendentals=0
        ),
        name="spin",
    )(strides, start)


def small_turn(x):
    y = x * x
    cosine = 1.0 - y * (0.5 - y * (1.0 / 24.0 - y * (1.0 / 720.0)))
    return cosine, x * (1.0 - y * (1.0 / 6.0 - y * (1.0 / 120.0 - y * (1.0 / 5040.0))))


def prepare(steer, angles, me, groups, ranks, rows, samples, pair, unit):
    members = steer[0].shape[1]
    smem = pl.BlockSpec(memory_space=pltpu.SMEM)
    vmem = pl.BlockSpec(memory_space=pltpu.VMEM)
    return pl.pallas_call(
        functools.partial(prepare_kernel, groups, ranks, rows, samples, pair),
        out_shape=[
            jax.ShapeDtypeStruct((groups, 2 * angles, 2 * members), BF16),
            jax.ShapeDtypeStruct((groups, angles, angles), BF16),
            jax.ShapeDtypeStruct((groups, 2, angles, LANES), F32),
            jax.ShapeDtypeStruct((unit // pair, groups, 2, angles, pair * LANES), F32),
        ],
        in_specs=[smem] + [vmem] * len(steer),
        out_specs=[vmem] * 4,
        compiler_params=pltpu.CompilerParams(vmem_limit_bytes=32 * 1024 * 1024),
        cost_estimate=pl.CostEstimate(
            flops=groups * angles * members * 40000, bytes_accessed=8 << 20, transcendentals=0
        ),
        name="prepare",
    )(me, *steer)


BAND = 32


def direct(source):
    return source & (source - 1) == 0


def kinds(groups):
    whole = [p for p in range(groups // 2) if direct(2 * p) and direct(2 * p + 1)]
    half = [p for p in range(groups // 2) if direct(2 * p) and not direct(2 * p + 1)]
    return whole, half


def columns(parts, wide, base, pair):
    return jnp.concatenate(
        [
            jnp.concatenate(
                [
                    ref[:, pl.ds(pl.multiple_of((base + u) * wide, 8), wide), :].reshape(-1, LANES)
                    for ref in parts
                ],
                axis=0,
            )
            for u in range(pair)
        ],
        axis=1,
    )


def rotated(mixed, turns, at, n, level, top, angles):
    band = slice(top, top + BAND)
    lower = slice(angles + top, angles + top + BAND)
    now = (turns[at, n, 0, band], turns[at, n, 1, band])
    power = twice(now) if level else now
    for _ in range(level - 1):
        power = complex_times(power, now)
    return complex_times((mixed[n, band], mixed[n, lower]), power)


def add(a, b):
    return a[0] + b[0], a[1] + b[1]


def near_kernel(groups, count, layout, mixes, turns, *refs):
    image, partial, mixed = refs[-3:]
    held = split(refs[:-3], layout)
    whole, half = kinds(groups)
    pair, angles = turns.shape[-1] // LANES, turns.shape[-2]
    wide = held[0][0].shape[1] // (count * pair)

    @pl.loop(0, count)
    def _(step):
        here = step
        cells = {o: columns(parts, wide, step * pair, pair) for o, parts in held.items()}
        ready = [n for n in range(groups) if direct(n)]
        for n in ready:
            mixed[n] = dot(mixes[n], cells[n])
        for pick in range(groups // 2):
            terms = [n for n in (2 * pick, 2 * pick + 1) if n in ready]
            for top in range(0, angles if terms else 0, BAND):
                band = slice(top, top + BAND)
                total = rotated(mixed, turns, here, terms[0], 0, top, angles)
                if len(terms) == 2:
                    total = add(total, rotated(mixed, turns, here, terms[1], 0, top, angles))
                    side = pair * LANES
                    image[step, whole.index(pick), band, :side] = total[0].astype(BF16)
                    image[step, whole.index(pick), band, side:] = total[1].astype(BF16)
                else:
                    spot = half.index(pick)
                    partial[step, spot, 0, band], partial[step, spot, 1, band] = total


def far_kernel(groups, count, layout, unit, mixes, mats, turns, image, partial, *refs):
    out, mixed, images = refs[-3:]
    held = split(refs[: sum(len(parts) for parts in layout.values())], layout)
    levels = groups.bit_length() - 1
    whole, half = kinds(groups)
    pair, angles = turns.shape[-1] // LANES, turns.shape[-2]
    wide = held[groups - 1][0].shape[1] // (count * pair)
    side = pair * LANES
    started = pl.program_id(0) * (unit // pair)
    middle = angles // 2
    window = min(angles, -(-(middle + REACH) // LANES) * LANES)
    if len(out.shape) == 3:
        out = out.reshape(out.shape[0] * out.shape[1], LANES)

    @pl.loop(0, unit // pair)
    def _(step):
        place = started + step
        here = place
        cells = {o: columns(parts, wide, place * pair, pair) for o, parts in held.items()}
        late = [n for n in range(groups) if n in held]
        for n in late:
            mixed[n] = dot(mixes[n], cells[n])
        for pick in range(groups // 2):
            terms = [n for n in (2 * pick, 2 * pick + 1) if n in late]
            if not terms:
                images[pick] = image[place, whole.index(pick)]
                continue
            for top in range(0, angles, BAND):
                band = slice(top, top + BAND)
                total = rotated(mixed, turns, here, terms[0], 0, top, angles)
                if len(terms) == 2:
                    total = add(total, rotated(mixed, turns, here, terms[1], 0, top, angles))
                else:
                    spot = half.index(pick)
                    total = add(total, (partial[place, spot, 0, band], partial[place, spot, 1, band]))
                images[pick, band, :side] = total[0].astype(BF16)
                images[pick, band, side:] = total[1].astype(BF16)
        for level in range(1, levels):
            last = level == levels - 1
            stride = 2 << level
            for offset in range(0, groups, stride):
                for h in range(2):
                    n = offset + h
                    source = images.at[(offset ^ (h << level)) // 2]
                    for low, high, start in ((0, middle, 0), (middle, angles, angles - window)):
                        turned = dot(mats[n, low:high, start : start + window], source[start : start + window])
                        mixed[n, low:high] = turned[:, :side]
                        mixed[n, angles + low : angles + high] = turned[:, side:]
            for offset in range(0, groups, stride):
                for top in range(0, angles, BAND):
                    band = slice(top, top + BAND)
                    re, im = add(
                        rotated(mixed, turns, here, offset, level, top, angles),
                        rotated(mixed, turns, here, offset + 1, level, top, angles),
                    )
                    if not last:
                        images[offset // 2, band, :side] = re.astype(BF16)
                        images[offset // 2, band, side:] = im.astype(BF16)
                        continue
                    for u in range(pair):
                        lanes = slice(u * LANES, (u + 1) * LANES)
                        spot = top * unit * 2 + (step * pair + u) * 2
                        out[pl.ds(spot, BAND, stride=unit * 2), :] = re[:, lanes]
                        out[pl.ds(spot + 1, BAND, stride=unit * 2), :] = im[:, lanes]


def split(refs, layout):
    held, at = {}, 0
    for offset, parts in layout.items():
        held[offset] = refs[at : at + len(parts)]
        at += len(parts)
    return held


def merge_near(held, mixes, turns, low, high):
    groups, pair, angles = mixes.shape[0], turns.shape[-1] // LANES, turns.shape[-2]
    vmem = pl.BlockSpec(memory_space=pltpu.VMEM)
    count = (high - low) // pair
    whole, half = kinds(groups)
    flat = [part for parts in held.values() for part in parts]
    return pl.pallas_call(
        functools.partial(near_kernel, groups, count, held),
        out_shape=[
            jax.ShapeDtypeStruct((count, len(whole), angles, 2 * pair * LANES), BF16),
            jax.ShapeDtypeStruct((count, len(half), 2, angles, pair * LANES), F32),
        ],
        in_specs=[vmem] * (2 + len(flat)),
        out_specs=[vmem] * 2,
        scratch_shapes=[pltpu.VMEM((groups, 2 * angles, pair * LANES), F32)],
        compiler_params=pltpu.CompilerParams(vmem_limit_bytes=MERGE_LIMIT),
        cost_estimate=pl.CostEstimate(
            flops=groups * angles * angles * (high - low) * LANES * 4,
            bytes_accessed=angles * (high - low) * LANES * 8,
            transcendentals=0,
        ),
        name="merge_near",
    )(mixes, turns, *flat)


def merge_far(held, mixes, mats, turns, image, partial, rows, low, high, unit, before):
    groups, pair, angles = mixes.shape[0], turns.shape[-1] // LANES, turns.shape[-2]
    vmem = pl.BlockSpec(memory_space=pltpu.VMEM)
    flat = [part for parts in held.values() for part in parts]
    if unit * 2 % 8:
        shape, block, spot = (angles * rows * 2, LANES), (angles * unit * 2, LANES), lambda i: (0, 0)
    else:
        shape, block = (angles, rows * 2, LANES), (angles, unit * 2, LANES)
        spot = lambda i: (0, low // unit + i, 0)
    operands = [mixes, mats, turns, image, partial, *flat]
    specs = [vmem] * len(operands)
    aliases = {}
    if before is not None:
        aliases[len(operands)] = 0
        operands.append(before)
        specs.append(pl.BlockSpec(memory_space=pltpu.HBM))
    return pl.pallas_call(
        functools.partial(far_kernel, groups, (high - low) // pair, held, unit),
        grid=((high - low) // unit,),
        out_shape=jax.ShapeDtypeStruct(shape, F32),
        in_specs=specs,
        out_specs=pl.BlockSpec(block, spot),
        input_output_aliases=aliases,
        scratch_shapes=[
            pltpu.VMEM((groups, 2 * angles, pair * LANES), F32),
            pltpu.VMEM((groups // 2, angles, 2 * pair * LANES), BF16),
        ],
        compiler_params=pltpu.CompilerParams(vmem_limit_bytes=MERGE_LIMIT),
        cost_estimate=pl.CostEstimate(
            flops=groups * angles * angles * (high - low) * LANES * 4,
            bytes_accessed=angles * (high - low) * LANES * 16,
            transcendentals=0,
        ),
        name="merge_far",
    )(*operands)


def hop(value, axis, offset):
    if not offset:
        return value
    return lax.ppermute(value, axis, [(i, i ^ offset) for i in range(lax.axis_size(axis))])


def neighbours(x, groups):
    return {1 << b: hop(x, "sub", 1 << b) for b in range(groups.bit_length() - 1)}


def others(x, near, groups):
    held = {0: [x]}
    for bit in near:
        held[bit] = [near[bit]]
    slots = x.shape[0]
    for offset in range(groups):
        if offset in held:
            continue
        via = [bit for bit in near if offset & bit]
        edges = [slots * i // len(via) for i in range(len(via) + 1)]
        pieces = []
        for bit, low, high in zip(via, edges[:-1], edges[1:]):
            source = held[offset ^ bit]
            source = source[0] if len(source) == 1 else jnp.concatenate(source, axis=0)
            pieces.append(hop(source[low:high], "sub", bit))
        held[offset] = pieces
    return [held[offset] for offset in range(groups)]


def local(echoes, filter_spectrum, range_shifts, steering, tap_offsets, tap_weights, phase_rates):
    ranks, groups = lax.axis_size("rng"), lax.axis_size("sub")
    pulses, _, samples = echoes.shape
    rows = samples // LANES // ranks
    angles = steering.shape[2]
    me = lax.axis_index("rng").astype(jnp.int32).reshape(1)
    unit = UNIT if rows % UNIT == 0 else rows
    cuts = [(low, low + unit) for low in range(0, rows, unit)]
    batches = [(0, unit)] + ([(unit, rows)] if unit < rows else [])

    near, odd, early = compress(
        echoes, filter_spectrum, range_shifts, steering, tap_offsets, tap_weights, phase_rates,
        me, ranks,
    )
    steers = [hop(early, "sub", e) for e in range(groups)]
    wide = 2 * pulses
    packed = pack(near, hop(odd, "rng", 1), batches, wide)
    batch = []
    for blocks in packed:
        batch.append([hop(block, "rng", 2 * z) for z, block in enumerate(blocks)])
    arrived = [jnp.concatenate(batch[0], axis=0)]
    steers, _ = lax.optimization_barrier((steers, arrived[0]))
    pair = 2 if unit % 2 == 0 else 1
    ready = prepare(steers, angles, me, groups, ranks, rows, samples, pair, unit)
    if len(batch) > 1:
        batch[1], ready = lax.optimization_barrier((batch[1], ready))
        for at in range(0, batch[1][0].shape[1], unit * wide):
            pieces = [piece[:, at : at + unit * wide] for piece in batch[1]]
            arrived.append(jnp.concatenate(pieces, axis=0))
    mixes, mats, strides, *turns = ready

    nears = []
    for x in arrived:
        nears.append(neighbours(x, groups))
    out = None
    for cut, (low, high) in enumerate(cuts):
        held = others(arrived[cut], nears[cut], groups)
        close = {o: held[o] for o in range(groups) if direct(o)}
        far = {o: held[o] for o in range(groups) if not direct(o)}
        image, partial = merge_near(close, mixes, turns[cut], low, high)
        if cut and cut + 1 < len(cuts):
            nears[cut + 1], image = lax.optimization_barrier((nears[cut + 1], image))
        out = merge_far(far, mixes, mats, turns[cut], image, partial, rows, low, high, unit, out)
        if not cut and len(cuts) > 1:
            strides, out = lax.optimization_barrier((strides, out))
            turns += spin(strides, turns[0], len(cuts) - 1)
            nears[1], turns[1], out = lax.optimization_barrier((nears[1], turns[1], out))
    out = out.reshape(angles, rows, 2, LANES).transpose(0, 2, 1, 3)
    out = with_layout_constraint(out, Layout(major_to_minor=(0, 2, 1, 3)))
    return out.reshape(angles, 2, rows * LANES)


def solution(mesh):
    placed = (
        P(("sub", "rng"), None, None),
        P(),
        P("sub"),
        P("sub", None, None, None),
        P("sub", None, None),
        P("sub", None, None, None),
        P("sub", None, None),
    )

    return jax.shard_map(
        local, mesh=mesh, in_specs=placed, out_specs=P("sub", None, "rng"), check_vma=False
    )
```
